32 devices in a mesh: cells: 16 (over z, x, core), ens: 2 (over y).
Axes of the slice: x: 2, y: 2, z: 4, core: 2. Of those that a mesh axis runs over, the one named last changes fastest.
Arguments:
- later_adjoint: float32 [4, 4, 32, 8, 128], P('ens', None, 'cells'), may hold values from -6 to 6
- coupling: bfloat16 [4, 6, 4, 4, 32, 8, 128], P('ens', None, None, None, 'cells'), may hold values from -0.59765625 to 0.59765625
- diag_inverse: bfloat16 [4, 4, 4, 32, 8, 128], P('ens', None, None, 'cells'), may hold values from -0.7 to 1.6, as said below
- sensitivity: bfloat16 [4, 4, 32, 8, 128, 128], P('ens', None, 'cells'), may hold values from -0.0625 to 0.0625
- well_cells: int32 [256], replicated, may hold values from 0 to 32767
- well_misfit: float32 [4, 4, 256], P('ens'), may hold values from -6 to 6
- block_map: int32 [32, 8, 128], P('cells'), may hold values from 0 to 63, as said below
Outputs:
- adjoint: float32 [4, 4, 32, 8, 128], P('ens', None, 'cells')
- gradient: float32 [64, 128], P('cells')
The draws below stay inside these ranges and needn't reach their ends.
Inputs may be any that keep to these rules, and one draw needn't show every extreme that they name: `block_map`: of the cells of each slab of 2 planes along the first dimension (x from i * 2 to i * 2 + 1), exactly 128 map to blocks whose number divided by 4 (rounded down) equals any given j. `diag_inverse`: each block is the inverse of a diagonal block; its diagonal entries lie in 0.4 to 1.6. `well_cells`: wells may share a cell.
All inputs are finite; a program needn't handle non-finite values.
Results may differ from the reference program's by a relative error of at most 0.0003.
Values sent between devices are 32-bit elements; how exact they have to be, the bound alone decides.
A program may use at most 64 MiB of HBM per device.

```python
import jax
import jax.numpy as jnp
from jax import lax

UNK = 4
PBLK = 128
CX = 2
NY = 8
NZ = 128
ITERS = 4
WELLS = 256
BLK_DEV = 4
MEMBERS = 4
NX = 32
NBLK = 64
N_CELLS = 16


def draw_diag_inverse(key, part):
    shape = (MEMBERS, UNK, UNK, NX, NY, NZ)
    identity = jnp.eye(UNK, dtype=jnp.float32)[None, :, :, None, None, None]
    key_diag = jax.random.fold_in(key, 21)
    key_off = jax.random.fold_in(key, 22)
    diagonal = jax.random.uniform(key_diag, shape, jnp.float32, 0.6, 1.4)
    offdiag = jnp.clip(0.2 * jax.random.normal(key_off, shape, jnp.float32), -0.7, 0.7)
    return (identity * diagonal + (1.0 - identity) * offdiag).astype(jnp.bfloat16)


def draw_block_map(key, part):
    slab_cells = CX * NY * NZ
    per_owner = slab_cells // N_CELLS
    owners = jnp.repeat(jnp.arange(N_CELLS, dtype=jnp.int32), per_owner)
    keys = jax.random.split(jax.random.fold_in(key, 31), N_CELLS)
    shuffled = jax.vmap(lambda single: jax.random.permutation(single, owners))(keys)
    within = jax.random.randint(jax.random.fold_in(key, 32), (N_CELLS, slab_cells), 0, BLK_DEV, dtype=jnp.int32)
    return (shuffled * BLK_DEV + within).reshape(NX, NY, NZ)


def plant(entries, stream_key, low, high):
    longest = entries.shape.index(max(entries.shape))
    spots = []
    for shift in (0, 1):
        where = [jax.random.randint(jax.random.fold_in(stream_key, axis), (), 0, length) for axis, length in enumerate(entries.shape)]
        where[longest] = (where[longest] + shift) % entries.shape[longest]
        spots.append(tuple(where))
    return entries.at[spots[0]].set(low).at[spots[1]].set(high)


def level_of(rng, shape, cuts, smallest, largest):
    def one(position, blocks):
        heights = jax.random.uniform(jax.random.fold_in(jax.random.fold_in(rng, 6), position), (blocks,), jnp.float32, smallest / len(cuts), largest / len(cuts))
        return jnp.repeat(jnp.exp(heights), shape[position] // blocks).reshape((-1,) + (1,) * (len(shape) - position - 1))

    loudness = one(*cuts[0])
    for cut in cuts[1:]:
        loudness = loudness * one(*cut)
    return loudness


def scatter_about(own_key, shape, width, most, cuts=(), kind=jnp.bfloat16):
    factor_of = level_of(own_key, shape, cuts, -0.22, 0.18) if cuts else 1.0
    result = jax.random.normal(own_key, shape, jnp.float32) * width * factor_of
    return jnp.minimum(jnp.maximum(result, -most), most).astype(kind)


def setup_inputs(seed: int = 0) -> dict:
    splits = jax.random.split(jax.random.key(seed), 8)
    later_adjoint = scatter_about(splits[0], (MEMBERS, UNK, NX, NY, NZ), 1.0, 6.0, ((0, 2), (2, 16)), jnp.float32)
    coupling = scatter_about(splits[1], (MEMBERS, 6, UNK, UNK, NX, NY, NZ), 0.1, 0.59765625, ((0, 2), (4, 16)))
    diag_inverse = draw_diag_inverse(jax.random.fold_in(splits[7], 71), 0)
    sensitivity = scatter_about(splits[3], (MEMBERS, UNK, NX, NY, NZ, PBLK), (UNK * MEMBERS * CX * NY * NZ // BLK_DEV) ** -0.5, 0.0625, ((0, 2), (2, 16)))
    well_cells = plant(jax.random.randint(splits[4], (WELLS,), 0, NX * NY * NZ), jax.random.fold_in(splits[4], 1), 0, (NX * NY * NZ) - 1).astype(jnp.int32)
    well_misfit = scatter_about(splits[5], (MEMBERS, UNK, WELLS), 1.0, 6.0, ((0, 2),), jnp.float32)
    block_map = draw_block_map(jax.random.fold_in(splits[7], 71), 0)
    return {"later_adjoint": later_adjoint, "coupling": coupling, "diag_inverse": diag_inverse, "sensitivity": sensitivity, "well_cells": well_cells, "well_misfit": well_misfit, "block_map": block_map}


def move_along(field, axis, forward):
    length = field.shape[axis]
    shape = list(field.shape)
    shape[axis] = 1
    zeros = jnp.zeros(shape, jnp.float32)
    if forward:
        return jnp.concatenate([zeros, lax.slice_in_dim(field, 0, length - 1, axis=axis)], axis=axis)
    return jnp.concatenate([lax.slice_in_dim(field, 1, length, axis=axis), zeros], axis=axis)


def coupling_sum(adjoint, coupling):
    terms = jnp.sum(coupling.astype(jnp.float32) * adjoint[:, None, :, None], axis=2)
    total = jnp.zeros(adjoint.shape, jnp.float32)
    directions = [(2, True), (2, False), (3, True), (3, False), (4, True), (4, False)]
    for number, (axis, forward) in enumerate(directions):
        total = total + move_along(terms[:, number], axis, forward)
    return total


def apply_inverse(diag_inverse, source):
    return jnp.sum(diag_inverse.astype(jnp.float32) * source[:, :, None], axis=1)


def reference(later_adjoint, coupling, diag_inverse, sensitivity, well_cells, well_misfit, block_map):
    members = later_adjoint.shape[0]
    count = NX * NY * NZ
    flat = later_adjoint.reshape(members, UNK, count)
    flat = flat.at[:, :, well_cells].add(well_misfit)
    source = flat.reshape(later_adjoint.shape)
    adjoint = apply_inverse(diag_inverse, source)
    for sweep in range(ITERS):
        adjoint = apply_inverse(diag_inverse, source - coupling_sum(adjoint, coupling))
    adjoint_flat = adjoint.reshape(members, UNK, count)
    sens_flat = sensitivity.reshape(members, UNK, count, PBLK)
    cell_grad = jnp.zeros((count, PBLK), jnp.float32)
    for member in range(members):
        for unknown in range(UNK):
            cell_grad = cell_grad + adjoint_flat[member, unknown][:, None] * sens_flat[member, unknown].astype(jnp.float32)
    gradient = jax.ops.segment_sum(cell_grad, block_map.reshape(-1), num_segments=NBLK)
    return adjoint, gradient
```

```python
import functools

import jax
import jax.numpy as jnp
from jax import lax
from jax.experimental import pallas as pl
from jax.experimental.pallas import tpu as pltpu
from jax.sharding import PartitionSpec as P

ITERS = 4
MESH = pl.DeviceIdType.MESH
F32 = jnp.float32
BF16 = jnp.bfloat16


def for_each(count, step):
    if count <= 64:
        for i in range(count):
            step(i)
    else:
        def body(i, carry):
            step(i)
            return carry

        lax.fori_loop(0, count, body, 0)


def split(value):
    high = value.astype(BF16).astype(F32)
    return high, value - high


def kernel(
    ranks, groups, blocks,
    later_hbm, coup_hbm, diag_hbm, sens_hbm, wells_hbm, misfit_hbm, map_hbm,
    adj, got_out,
    later, coup, diag, sens, wells, misfit, bmap, source,
    out_buf, in_buf, mid_edge, last_edge, left, mask, part, got,
    load_sem, recv_sem, send_sem, part_ssem, part_rsem, here_sem,
):
    members, unknowns, planes, columns, layers = later.shape
    rows = planes * columns
    count = rows * layers
    devices = ranks * groups
    blk_dev = blocks // ranks
    fields = members * unknowns
    me_c = lax.axis_index("cells")
    me_e = lax.axis_index("ens")
    me = me_c * groups + me_e
    assert planes >= 2

    loads = [
        pltpu.make_async_copy(src, dst, load_sem.at[i])
        for i, (src, dst) in enumerate(
            [
                (wells_hbm, wells), (misfit_hbm, misfit), (later_hbm, later), (diag_hbm, diag),
                (coup_hbm.at[:, 0:2], coup.at[:, 0:2]), (coup_hbm.at[:, 2:6], coup.at[:, 2:6]),
                (map_hbm, bmap), (sens_hbm, sens),
            ]
        )
    ]
    for load in loads[:7]:
        load.start()

    barrier = pltpu.get_barrier_semaphore()
    block_c = 1
    while (block_c * groups) ** 2 < devices:
        block_c *= 2
    columns_c = ranks // block_c

    def wrap(at, size):
        return jnp.where(at >= size, at - size, at)

    pos_c = lax.rem(me_c, block_c)
    base_c = me_c - pos_c
    near = [
        (base_c + wrap(pos_c + dc, block_c), wrap(me_e + de, groups))
        for dc in range(block_c) for de in range(groups) if dc or de
    ]
    far = [(wrap(me_c + block_c * s, ranks), me_e) for s in range(1, columns_c)]
    cross_up = (pos_c == block_c - 1) & (me_c < ranks - 1)
    cross_down = (pos_c == 0) & (me_c > 0)
    next_id = (jnp.minimum(me_c + 1, ranks - 1), me_e)
    prev_id = (jnp.maximum(me_c - 1, 0), me_e)

    def greet(who):
        pl.semaphore_signal(barrier, inc=1, device_id=who, device_id_type=MESH)

    for who in near + far:
        greet(who)

    @pl.when(cross_up)
    def _():
        greet(next_id)

    @pl.when(cross_down)
    def _():
        greet(prev_id)

    def greeted():
        extra = jnp.where(cross_up, 1, 0) + jnp.where(cross_down, 1, 0)
        pl.semaphore_wait(barrier, len(near) + len(far) + extra)

    has = (me_c > 0, me_c < ranks - 1)
    target = (prev_id, next_id)
    edge_at = (0, planes - 1)
    turn = lax.rem(me_c, 4)
    patient = (turn == 2, turn == 1)
    GAIN = 4

    def remote(d, src, dst, sem):
        return pltpu.make_async_remote_copy(
            src_ref=src, dst_ref=dst, send_sem=send_sem.at[d], recv_sem=sem,
            device_id=target[d], device_id_type=MESH,
        )

    def value_copy(d, slot, m):
        return remote(d, out_buf.at[d, slot, m], in_buf.at[1 - d, slot, m], recv_sem.at[1 - d, slot, m])

    def gain_copy(d, m):
        both = pl.ds(GAIN, unknowns)
        return remote(d, out_buf.at[d, both, m], in_buf.at[1 - d, both, m], recv_sem.at[1 - d, GAIN, m])

    def value_wait(d, slot, m):
        pltpu.make_async_remote_copy(
            src_ref=out_buf.at[d, slot, m], dst_ref=in_buf.at[d, slot, m], send_sem=send_sem.at[d],
            recv_sem=recv_sem.at[d, slot, m], device_id=next_id, device_id_type=MESH,
        ).wait_recv()

    def gain_wait(d, m):
        both = pl.ds(GAIN, unknowns)
        pltpu.make_async_remote_copy(
            src_ref=out_buf.at[d, both, m], dst_ref=in_buf.at[d, both, m], send_sem=send_sem.at[d],
            recv_sem=recv_sem.at[d, GAIN, m], device_id=next_id, device_id_type=MESH,
        ).wait_recv()

    for d in range(2):
        @pl.when(jnp.logical_not(has[d]))
        def _(d=d):
            in_buf[d] = jnp.zeros(in_buf.shape[1:], F32)

    loads[0].wait()
    loads[1].wait()
    total_wells = wells.shape[1]
    rel = wells[...] - me_c * count
    row_lo = lax.broadcasted_iota(jnp.int32, (rows, total_wells), 0) * layers
    in_row = (rel >= row_lo) & (rel < row_lo + layers)
    lane = wells[...] & (layers - 1)
    at_lane = lax.broadcasted_iota(jnp.int32, (layers, total_wells), 0) == lane
    at_lane = jnp.where(at_lane, 1.0, 0.0).astype(BF16)
    parts = [[], [], []]
    for m in range(members):
        for u in range(unknowns):
            rest = jnp.broadcast_to(misfit[m, u : u + 1, :], (rows, total_wells))
            rest = jnp.where(in_row, rest, 0.0)
            for i in range(3):
                high, rest = split(rest)
                parts[i].append(high.astype(BF16))
    injected = jnp.zeros((fields * rows, layers), F32)
    for piece in parts:
        injected = injected + lax.dot_general(
            jnp.concatenate(piece, axis=0), at_lane, (((1,), (1,)), ((), ())),
            preferred_element_type=F32,
        )
    loads[2].wait()
    source[...] = later[...] + injected.reshape(later.shape)

    def weighed(weights, values):
        out = None
        for w in range(unknowns):
            term = weights(w) * values[w][None]
            out = term if out is None else out + term
        return out

    def inverse(m, rhs):
        return weighed(lambda w: diag[m, w].astype(F32), rhs)

    loads[3].wait()
    loads[4].wait()

    def own_gain(d, m, values):
        return weighed(lambda w: out_buf[d, GAIN + w, m], values)

    def far_gain(d, m, values):
        return weighed(lambda w: in_buf[d, GAIN + w, m], values)

    for m in range(members):
        for d in range(2):
            at = edge_at[d]
            for w in range(unknowns):
                out_buf[d, GAIN + w, m] = weighed(
                    lambda u: coup[m, 1 - d, u, :, at].astype(F32), diag[m, w, :, at].astype(F32)
                )
    edge = [[None, None] for _ in range(members)]
    for m in range(members):
        for d in range(2):
            edge[m][d] = own_gain(d, m, source[m, :, edge_at[d]])
            out_buf[d, 0, m] = edge[m][d]
    greeted()

    def send(d, copy, when):
        @pl.when(has[d] & when if when is not None else has[d])
        def _():
            copy.start()

    hasty = tuple(jnp.logical_not(p) for p in patient)
    for m in range(members):
        for d in range(2):
            send(d, value_copy(d, 0, m), None)
    for m in range(members):
        for d in range(2):
            send(d, gain_copy(d, m), hasty[d])
    for who in far:
        pl.semaphore_signal(here_sem, inc=1, device_id=who, device_id_type=MESH)

    now = [inverse(m, source[m]) for m in range(members)]

    lane_at = lax.broadcasted_iota(jnp.int32, (unknowns, planes, columns, layers), 3)
    col_at = lax.broadcasted_iota(jnp.int32, (unknowns, planes, columns, layers), 2)

    def product(m, k, value, lo, hi):
        return weighed(lambda u: coup[m, k, u, :, lo:hi].astype(F32), value[:, lo:hi])

    def inside(m, value):
        moved = pltpu.roll(product(m, 2, value, 0, planes), 1, 2)
        total = jnp.where(col_at == 0, 0.0, moved)
        moved = pltpu.roll(product(m, 3, value, 0, planes), columns - 1, 2)
        total = total + jnp.where(col_at == columns - 1, 0.0, moved)
        moved = pltpu.roll(product(m, 4, value, 0, planes), 1, 3)
        total = total + jnp.where(lane_at == 0, 0.0, moved)
        moved = pltpu.roll(product(m, 5, value, 0, planes), layers - 1, 3)
        total = total + jnp.where(lane_at == layers - 1, 0.0, moved)
        up = product(m, 0, value, 0, planes - 1)
        down = product(m, 1, value, 1, planes)
        nothing = jnp.zeros((unknowns, 1, columns, layers), F32)
        total = total + jnp.concatenate([nothing, up], axis=1)
        total = total + jnp.concatenate([down, nothing], axis=1)
        return source[m] - total

    def ahead(d, slot, m, rest):
        out_buf[d, slot, m] = own_gain(d, m, rest[:, edge_at[d]])

    def subtract(rest, below, above):
        first_plane = rest[:, 0] - below
        last_plane = rest[:, planes - 1] - above
        return jnp.concatenate(
            [first_plane[:, None], rest[:, 1 : planes - 1], last_plane[:, None]], axis=1
        ) if planes > 2 else jnp.stack([first_plane, last_plane], axis=1)

    loads[5].wait()
    loads[7].start()
    rest = [inside(m, now[m]) for m in range(members)]
    for m in range(members):
        for d in range(2):
            @pl.when(hasty[d])
            def _(d=d, m=m):
                ahead(d, 1, m, rest[m])

            send(d, value_copy(d, 1, m), hasty[d])

    loads[6].wait()
    ids = lax.broadcasted_iota(jnp.int32, (blocks, layers), 0)
    for x in range(planes):
        for y in range(columns):
            hit = jnp.where(bmap[x, y : y + 1, :] == ids, 1.0, 0.0)
            mask[x, y] = hit.astype(BF16)

    first_edge = edge
    second_edge = [[None, None] for _ in range(members)]
    for m in range(members):
        for d in range(2):
            @pl.when(has[d])
            def _(d=d, m=m):
                value_wait(d, 0, m)
        given = subtract(rest[m], in_buf[0, 0, m], in_buf[1, 0, m])
        for d in range(2):
            second_edge[m][d] = own_gain(d, m, given[:, edge_at[d]])

            @pl.when(patient[d])
            def _(d=d, m=m):
                out_buf[d, 1, m] = second_edge[m][d]

            send(d, value_copy(d, 1, m), patient[d])
        now[m] = inverse(m, given)
        rest[m] = inside(m, now[m])
        for d in range(2):
            ahead(d, 2, m, rest[m])
            send(d, value_copy(d, 2, m), None)
    for m in range(members):
        for d in range(2):
            send(d, gain_copy(d, m), patient[d])

    for m in range(members):
        for d in range(2):
            @pl.when(has[d])
            def _(d=d, m=m):
                value_wait(d, 1, m)

            @pl.when(has[d] & hasty[d])
            def _(d=d, m=m):
                gain_wait(d, m)

            @pl.when(hasty[d])
            def _(d=d, m=m):
                mid_edge[d, m] = in_buf[d, 1, m] - far_gain(d, m, first_edge[m][d])

            @pl.when(patient[d])
            def _(d=d, m=m):
                mid_edge[d, m] = in_buf[d, 1, m]

        given = subtract(rest[m], mid_edge[0, m], mid_edge[1, m])
        for d in range(2):
            last_edge[d, m] = own_gain(d, m, given[:, edge_at[d]])
        now[m] = inverse(m, given)
        rest[m] = inside(m, now[m])
        for d in range(2):
            ahead(d, 3, m, rest[m])
            send(d, value_copy(d, 3, m), None)

    for m in range(members):
        for d in range(2):
            @pl.when(has[d])
            def _(d=d, m=m):
                value_wait(d, 2, m)

            @pl.when(has[d] & patient[d])
            def _(d=d, m=m):
                gain_wait(d, m)

        came_in = [in_buf[d, 2, m] - far_gain(d, m, second_edge[m][d]) for d in range(2)]
        now[m] = inverse(m, subtract(rest[m], *came_in))
        left[m] = inside(m, now[m])

    loads[7].wait()

    def finish(d, total):
        at = d * (planes - 1)
        for m in range(members):
            @pl.when(jnp.where(d == 0, me_c > 0, me_c < ranks - 1))
            def _(m=m):
                value_wait(d, 3, m)

        for m in range(members):
            came_in = in_buf[d, 3, m] - far_gain(d, m, last_edge[d, m])
            value = weighed(lambda w: diag[m, w, :, at].astype(F32), left[m, :, at] - came_in)
            adj[m, :, at] = value
        return gather(at, total)

    def gather(at, total):
        def field(i, total):
            m, u = i // unknowns, i % unknowns
            pieces = split(adj[m, u, at])
            lhs = []
            for value in pieces:
                part_lhs = []
                for y in range(columns):
                    wide = jnp.broadcast_to(value[y : y + 1], (16, layers)).astype(BF16)
                    wide = jnp.concatenate([wide] * (blocks // 16), axis=0)
                    part_lhs.append(mask[at, y] * wide)
                lhs.append(jnp.concatenate(part_lhs, axis=1))
            lhs = jnp.concatenate(lhs, axis=0)
            rhs = sens[i, pl.ds(at * columns, columns)].reshape(columns * layers, sens.shape[-1])
            return total + jnp.dot(lhs, rhs, preferred_element_type=F32)

        if blocks <= 64:
            for i in range(fields):
                total = field(i, total)
            return total
        return lax.fori_loop(0, fields, field, total)

    close = lax.rem(me_c + 1, 2)
    total = jnp.zeros((2 * blocks, sens.shape[-1]), F32)
    total = finish(close, total)
    for x in range(1, planes - 1):
        for m in range(members):
            adj[m, :, x] = weighed(lambda w: diag[m, w, :, x].astype(F32), left[m, :, x])
        total = gather(x, total)
    total = finish(1 - close, total)
    total = total[:blocks] + total[blocks:]
    for c in range(ranks):
        part[c] = total[c * blk_dev : (c + 1) * blk_dev]
    got[me] = part[me_c]

    def part_copy(c, e):
        return pltpu.make_async_remote_copy(
            src_ref=part.at[c], dst_ref=got.at[me], send_sem=part_ssem, recv_sem=part_rsem,
            device_id=(c, e), device_id_type=MESH,
        )

    pl.semaphore_wait(here_sem, len(far))

    def give(to):
        @pl.when(me != to)
        def _():
            part_copy(to // groups, to % groups).start()

    for_each(devices, give)
    others = got.at[pl.ds(0, devices - 1)]
    everything = pltpu.make_async_remote_copy(
        src_ref=others, dst_ref=others, send_sem=part_ssem, recv_sem=part_rsem,
        device_id=next_id, device_id_type=MESH,
    )
    everything.wait_recv()
    got_out[...] = jnp.sum(got[...], axis=0)

    everything.wait_send()
    for d in range(2):
        @pl.when(has[d])
        def _(d=d):
            pltpu.make_async_remote_copy(
                src_ref=out_buf.at[d], dst_ref=out_buf.at[d], send_sem=send_sem.at[d],
                recv_sem=send_sem.at[d], device_id=next_id, device_id_type=MESH,
            ).wait_send()


def write_out(adjoint, gradient, adjoint_hbm, gradient_hbm, sem):
    copies = [
        pltpu.make_async_copy(adjoint, adjoint_hbm, sem.at[0]),
        pltpu.make_async_copy(gradient, gradient_hbm, sem.at[1]),
    ]
    for copy in copies:
        copy.start()
    for copy in copies:
        copy.wait()


def solution(mesh):
    ranks, groups = mesh.shape["cells"], mesh.shape["ens"]
    assert (ranks * groups) & (ranks * groups - 1) == 0

    def body(later_adjoint, coupling, diag_inverse, sensitivity, well_cells, well_misfit, block_map):
        members, unknowns, planes, columns, layers = later_adjoint.shape
        params = sensitivity.shape[-1]
        rows = planes * columns
        blk_dev = 4
        blocks = ranks * blk_dev
        fields = members * unknowns
        sens = sensitivity.reshape(fields, rows, layers, params)
        wells = well_cells.reshape(1, -1)
        edge = (members, unknowns, columns, layers)
        any_spec = pl.BlockSpec(memory_space=pl.ANY)
        vmem_spec = pl.BlockSpec(memory_space=pltpu.VMEM)
        dma = pltpu.SemaphoreType.DMA
        adjoint, gradient = pl.pallas_call(
            functools.partial(kernel, ranks, groups, blocks),
            out_shape=(
                pltpu.VMEM(later_adjoint.shape, F32),
                pltpu.VMEM((blk_dev, params), F32),
            ),
            in_specs=[any_spec] * 7,
            out_specs=(vmem_spec, vmem_spec),
            scratch_shapes=[
                pltpu.VMEM(later_adjoint.shape, F32),
                pltpu.VMEM(coupling.shape, BF16),
                pltpu.VMEM(diag_inverse.shape, BF16),
                pltpu.VMEM(sens.shape, BF16),
                pltpu.VMEM(wells.shape, jnp.int32),
                pltpu.VMEM(well_misfit.shape, F32),
                pltpu.VMEM(block_map.shape, jnp.int32),
                pltpu.VMEM(later_adjoint.shape, F32),
                pltpu.VMEM((2, 4 + unknowns) + edge, F32),
                pltpu.VMEM((2, 4 + unknowns) + edge, F32),
                pltpu.VMEM((2,) + edge, F32),
                pltpu.VMEM((2,) + edge, F32),
                pltpu.VMEM(later_adjoint.shape, F32),
                pltpu.VMEM((planes, columns, blocks, layers), BF16),
                pltpu.VMEM((ranks, blk_dev, params), F32),
                pltpu.VMEM((ranks * groups, blk_dev, params), F32),
                dma((8,)),
                dma((2, 5, members)),
                dma((2,)),
                dma,
                dma,
                pltpu.SemaphoreType.REGULAR,
            ],
            compiler_params=pltpu.CompilerParams(collective_id=0, has_side_effects=True),
        )(later_adjoint, coupling, diag_inverse, sens, wells, well_misfit, block_map)
        return pl.pallas_call(
            write_out,
            out_shape=(
                jax.ShapeDtypeStruct(adjoint.shape, F32),
                jax.ShapeDtypeStruct(gradient.shape, F32),
            ),
            in_specs=[vmem_spec] * 2,
            out_specs=(any_spec, any_spec),
            scratch_shapes=[dma((2,))],
        )(*[pltpu.with_memory_space_constraint(a, pltpu.VMEM) for a in (adjoint, gradient)])

    placed = (
        P("ens", None, "cells", None, None),
        P("ens", None, None, None, "cells", None, None),
        P("ens", None, None, "cells", None, None),
        P("ens", None, "cells", None, None, None),
        P(),
        P("ens", None, None),
        P("cells", None, None),
    )
    return jax.shard_map(
        body,
        mesh=mesh,
        in_specs=placed,
        out_specs=(P("ens", None, "cells", None, None), P("cells", None)),
        check_vma=False,
    )
```

```python
import functools

import jax
import jax.numpy as jnp
from jax import lax
from jax.experimental import pallas as pl
from jax.experimental.pallas import tpu as pltpu
from jax.sharding import PartitionSpec as P

ITERS = 4
MESH = pl.DeviceIdType.MESH
F32 = jnp.float32
BF16 = jnp.bfloat16


def for_each(count, step):
    if count <= 64:
        for i in range(count):
            step(i)
    else:
        def body(i, carry):
            step(i)
            return carry

        lax.fori_loop(0, count, body, 0)


def split(value):
    high = value.astype(BF16).astype(F32)
    return high, value - high


def kernel(
    ranks, groups, blocks,
    later_hbm, coup_hbm, diag_hbm, sens_hbm, wells_hbm, misfit_hbm, map_hbm,
    adj, got_out,
    later, coup, diag, sens, wells, misfit, bmap, source,
    out_buf, in_buf, mid_edge, last_edge, left, mask, part, got,
    load_sem, recv_sem, send_sem, part_ssem, part_rsem, here_sem,
):
    members, unknowns, planes, columns, layers = later.shape
    rows = planes * columns
    count = rows * layers
    devices = ranks * groups
    blk_dev = blocks // ranks
    fields = members * unknowns
    me_c = lax.axis_index("cells")
    me_e = lax.axis_index("ens")
    me = me_c * groups + me_e
    assert planes >= 2

    loads = [
        pltpu.make_async_copy(src, dst, load_sem.at[i])
        for i, (src, dst) in enumerate(
            [
                (wells_hbm, wells), (misfit_hbm, misfit), (later_hbm, later), (diag_hbm, diag),
                (coup_hbm.at[:, 0:2], coup.at[:, 0:2]), (coup_hbm.at[:, 2:6], coup.at[:, 2:6]),
                (map_hbm, bmap), (sens_hbm, sens),
            ]
        )
    ]
    for load in loads[:7]:
        load.start()

    barrier = pltpu.get_barrier_semaphore()
    block_c = 1
    while (block_c * groups) ** 2 < devices:
        block_c *= 2
    columns_c = ranks // block_c

    def wrap(at, size):
        return jnp.where(at >= size, at - size, at)

    pos_c = lax.rem(me_c, block_c)
    base_c = me_c - pos_c
    near = [
        (base_c + wrap(pos_c + dc, block_c), wrap(me_e + de, groups))
        for dc in range(block_c) for de in range(groups) if dc or de
    ]
    far = [(wrap(me_c + block_c * s, ranks), me_e) for s in range(1, columns_c)]
    cross_up = (pos_c == block_c - 1) & (me_c < ranks - 1)
    cross_down = (pos_c == 0) & (me_c > 0)
    next_id = (jnp.minimum(me_c + 1, ranks - 1), me_e)
    prev_id = (jnp.maximum(me_c - 1, 0), me_e)

    def greet(who):
        pl.semaphore_signal(barrier, inc=1, device_id=who, device_id_type=MESH)

    for who in near + far:
        greet(who)

    @pl.when(cross_up)
    def _():
        greet(next_id)

    @pl.when(cross_down)
    def _():
        greet(prev_id)

    def greeted():
        extra = jnp.where(cross_up, 1, 0) + jnp.where(cross_down, 1, 0)
        pl.semaphore_wait(barrier, len(near) + len(far) + extra)

    has = (me_c > 0, me_c < ranks - 1)
    target = (prev_id, next_id)
    edge_at = (0, planes - 1)
    turn = lax.rem(me_c, 4)
    patient = (turn == 0, turn == 3)
    GAIN = 4

    def remote(d, src, dst, sem):
        return pltpu.make_async_remote_copy(
            src_ref=src, dst_ref=dst, send_sem=send_sem.at[d], recv_sem=sem,
            device_id=target[d], device_id_type=MESH,
        )

    def value_copy(d, slot, m):
        return remote(d, out_buf.at[d, slot, m], in_buf.at[1 - d, slot, m], recv_sem.at[1 - d, slot, m])

    def gain_copy(d, m):
        both = pl.ds(GAIN, unknowns)
        return remote(d, out_buf.at[d, both, m], in_buf.at[1 - d, both, m], recv_sem.at[1 - d, GAIN, m])

    def value_wait(d, slot, m):
        pltpu.make_async_remote_copy(
            src_ref=out_buf.at[d, slot, m], dst_ref=in_buf.at[d, slot, m], send_sem=send_sem.at[d],
            recv_sem=recv_sem.at[d, slot, m], device_id=next_id, device_id_type=MESH,
        ).wait_recv()

    def gain_wait(d, m):
        both = pl.ds(GAIN, unknowns)
        pltpu.make_async_remote_copy(
            src_ref=out_buf.at[d, both, m], dst_ref=in_buf.at[d, both, m], send_sem=send_sem.at[d],
            recv_sem=recv_sem.at[d, GAIN, m], device_id=next_id, device_id_type=MESH,
        ).wait_recv()

    for d in range(2):
        @pl.when(jnp.logical_not(has[d]))
        def _(d=d):
            in_buf[d] = jnp.zeros(in_buf.shape[1:], F32)

    loads[0].wait()
    loads[1].wait()
    total_wells = wells.shape[1]
    rel = wells[...] - me_c * count
    row_lo = lax.broadcasted_iota(jnp.int32, (rows, total_wells), 0) * layers
    in_row = (rel >= row_lo) & (rel < row_lo + layers)
    lane = wells[...] & (layers - 1)
    at_lane = lax.broadcasted_iota(jnp.int32, (layers, total_wells), 0) == lane
    at_lane = jnp.where(at_lane, 1.0, 0.0).astype(BF16)
    parts = [[], [], []]
    for m in range(members):
        for u in range(unknowns):
            rest = jnp.broadcast_to(misfit[m, u : u + 1, :], (rows, total_wells))
            rest = jnp.where(in_row, rest, 0.0)
            for i in range(3):
                high, rest = split(rest)
                parts[i].append(high.astype(BF16))
    injected = jnp.zeros((fields * rows, layers), F32)
    for piece in parts:
        injected = injected + lax.dot_general(
            jnp.concatenate(piece, axis=0), at_lane, (((1,), (1,)), ((), ())),
            preferred_element_type=F32,
        )
    loads[2].wait()
    source[...] = later[...] + injected.reshape(later.shape)

    def weighed(weights, values):
        out = None
        for w in range(unknowns):
            term = weights(w) * values[w][None]
            out = term if out is None else out + term
        return out

    def inverse(m, rhs):
        return weighed(lambda w: diag[m, w].astype(F32), rhs)

    loads[3].wait()
    loads[4].wait()

    def own_gain(d, m, values):
        return weighed(lambda w: out_buf[d, GAIN + w, m], values)

    def far_gain(d, m, values):
        return weighed(lambda w: in_buf[d, GAIN + w, m], values)

    for m in range(members):
        for d in range(2):
            at = edge_at[d]
            for w in range(unknowns):
                out_buf[d, GAIN + w, m] = weighed(
                    lambda u: coup[m, 1 - d, u, :, at].astype(F32), diag[m, w, :, at].astype(F32)
                )
    edge = [[None, None] for _ in range(members)]
    for m in range(members):
        for d in range(2):
            edge[m][d] = own_gain(d, m, source[m, :, edge_at[d]])
            out_buf[d, 0, m] = edge[m][d]
    greeted()

    def send(d, copy, when):
        @pl.when(has[d] & when if when is not None else has[d])
        def _():
            copy.start()

    hasty = tuple(jnp.logical_not(p) for p in patient)
    for m in range(members):
        for d in range(2):
            send(d, value_copy(d, 0, m), None)
    for who in far:
        pl.semaphore_signal(here_sem, inc=1, device_id=who, device_id_type=MESH)

    now = [inverse(m, source[m]) for m in range(members)]

    lane_at = lax.broadcasted_iota(jnp.int32, (unknowns, planes, columns, layers), 3)
    col_at = lax.broadcasted_iota(jnp.int32, (unknowns, planes, columns, layers), 2)

    def product(m, k, value, lo, hi):
        return weighed(lambda u: coup[m, k, u, :, lo:hi].astype(F32), value[:, lo:hi])

    def inside(m, value):
        moved = pltpu.roll(product(m, 2, value, 0, planes), 1, 2)
        total = jnp.where(col_at == 0, 0.0, moved)
        moved = pltpu.roll(product(m, 3, value, 0, planes), columns - 1, 2)
        total = total + jnp.where(col_at == columns - 1, 0.0, moved)
        moved = pltpu.roll(product(m, 4, value, 0, planes), 1, 3)
        total = total + jnp.where(lane_at == 0, 0.0, moved)
        moved = pltpu.roll(product(m, 5, value, 0, planes), layers - 1, 3)
        total = total + jnp.where(lane_at == layers - 1, 0.0, moved)
        up = product(m, 0, value, 0, planes - 1)
        down = product(m, 1, value, 1, planes)
        nothing = jnp.zeros((unknowns, 1, columns, layers), F32)
        total = total + jnp.concatenate([nothing, up], axis=1)
        total = total + jnp.concatenate([down, nothing], axis=1)
        return source[m] - total

    def ahead(d, slot, m, rest):
        out_buf[d, slot, m] = own_gain(d, m, rest[:, edge_at[d]])

    def subtract(rest, below, above):
        first_plane = rest[:, 0] - below
        last_plane = rest[:, planes - 1] - above
        return jnp.concatenate(
            [first_plane[:, None], rest[:, 1 : planes - 1], last_plane[:, None]], axis=1
        ) if planes > 2 else jnp.stack([first_plane, last_plane], axis=1)

    loads[5].wait()
    loads[7].start()
    rest = [inside(m, now[m]) for m in range(members)]
    for m in range(members):
        for d in range(2):
            @pl.when(hasty[d])
            def _(d=d, m=m):
                ahead(d, 1, m, rest[m])

            send(d, value_copy(d, 1, m), hasty[d])

    loads[6].wait()
    ids = lax.broadcasted_iota(jnp.int32, (blocks, layers), 0)
    for x in range(planes):
        for y in range(columns):
            hit = jnp.where(bmap[x, y : y + 1, :] == ids, 1.0, 0.0)
            mask[x, y] = hit.astype(BF16)

    for m in range(members):
        for d in range(2):
            send(d, gain_copy(d, m), hasty[d])

    first_edge = edge
    second_edge = [[None, None] for _ in range(members)]
    for m in range(members):
        for d in range(2):
            @pl.when(has[d])
            def _(d=d, m=m):
                value_wait(d, 0, m)
        given = subtract(rest[m], in_buf[0, 0, m], in_buf[1, 0, m])
        for d in range(2):
            second_edge[m][d] = own_gain(d, m, given[:, edge_at[d]])

            @pl.when(patient[d])
            def _(d=d, m=m):
                out_buf[d, 1, m] = second_edge[m][d]

            send(d, value_copy(d, 1, m), patient[d])
        now[m] = inverse(m, given)
        rest[m] = inside(m, now[m])
        for d in range(2):
            ahead(d, 2, m, rest[m])
            send(d, value_copy(d, 2, m), None)
    for m in range(members):
        for d in range(2):
            send(d, gain_copy(d, m), patient[d])

    for m in range(members):
        for d in range(2):
            @pl.when(has[d])
            def _(d=d, m=m):
                value_wait(d, 1, m)

            @pl.when(has[d] & hasty[d])
            def _(d=d, m=m):
                gain_wait(d, m)

            @pl.when(hasty[d])
            def _(d=d, m=m):
                mid_edge[d, m] = in_buf[d, 1, m] - far_gain(d, m, first_edge[m][d])

            @pl.when(patient[d])
            def _(d=d, m=m):
                mid_edge[d, m] = in_buf[d, 1, m]

        given = subtract(rest[m], mid_edge[0, m], mid_edge[1, m])
        for d in range(2):
            last_edge[d, m] = own_gain(d, m, given[:, edge_at[d]])
        now[m] = inverse(m, given)
        rest[m] = inside(m, now[m])
        for d in range(2):
            ahead(d, 3, m, rest[m])
            send(d, value_copy(d, 3, m), None)

    for m in range(members):
        for d in range(2):
            @pl.when(has[d])
            def _(d=d, m=m):
                value_wait(d, 2, m)

            @pl.when(has[d] & patient[d])
            def _(d=d, m=m):
                gain_wait(d, m)

        came_in = [in_buf[d, 2, m] - far_gain(d, m, second_edge[m][d]) for d in range(2)]
        now[m] = inverse(m, subtract(rest[m], *came_in))
        left[m] = inside(m, now[m])

    loads[7].wait()

    def finish(d, total):
        at = d * (planes - 1)
        for m in range(members):
            @pl.when(jnp.where(d == 0, me_c > 0, me_c < ranks - 1))
            def _(m=m):
                value_wait(d, 3, m)

        for m in range(members):
            came_in = in_buf[d, 3, m] - far_gain(d, m, last_edge[d, m])
            value = weighed(lambda w: diag[m, w, :, at].astype(F32), left[m, :, at] - came_in)
            adj[m, :, at] = value
        return gather(at, total)

    def gather(at, total):
        def field(i, total):
            m, u = i // unknowns, i % unknowns
            pieces = split(adj[m, u, at])
            lhs = []
            for value in pieces:
                part_lhs = []
                for y in range(columns):
                    wide = jnp.broadcast_to(value[y : y + 1], (16, layers)).astype(BF16)
                    wide = jnp.concatenate([wide] * (blocks // 16), axis=0)
                    part_lhs.append(mask[at, y] * wide)
                lhs.append(jnp.concatenate(part_lhs, axis=1))
            lhs = jnp.concatenate(lhs, axis=0)
            rhs = sens[i, pl.ds(at * columns, columns)].reshape(columns * layers, sens.shape[-1])
            return total + jnp.dot(lhs, rhs, preferred_element_type=F32)

        if blocks <= 64:
            for i in range(fields):
                total = field(i, total)
            return total
        return lax.fori_loop(0, fields, field, total)

    close = lax.rem(me_c + 1, 2)
    total = jnp.zeros((2 * blocks, sens.shape[-1]), F32)
    total = finish(close, total)
    for x in range(1, planes - 1):
        for m in range(members):
            adj[m, :, x] = weighed(lambda w: diag[m, w, :, x].astype(F32), left[m, :, x])
        total = gather(x, total)
    total = finish(1 - close, total)
    total = total[:blocks] + total[blocks:]
    for c in range(ranks):
        part[c] = total[c * blk_dev : (c + 1) * blk_dev]
    got[me] = part[me_c]

    def part_copy(c, e):
        return pltpu.make_async_remote_copy(
            src_ref=part.at[c], dst_ref=got.at[me], send_sem=part_ssem, recv_sem=part_rsem,
            device_id=(c, e), device_id_type=MESH,
        )

    pl.semaphore_wait(here_sem, len(far))

    def give(to):
        @pl.when(me != to)
        def _():
            part_copy(to // groups, to % groups).start()

    for_each(devices, give)
    others = got.at[pl.ds(0, devices - 1)]
    everything = pltpu.make_async_remote_copy(
        src_ref=others, dst_ref=others, send_sem=part_ssem, recv_sem=part_rsem,
        device_id=next_id, device_id_type=MESH,
    )
    everything.wait_recv()
    got_out[...] = jnp.sum(got[...], axis=0)

    everything.wait_send()
    for d in range(2):
        @pl.when(has[d])
        def _(d=d):
            pltpu.make_async_remote_copy(
                src_ref=out_buf.at[d], dst_ref=out_buf.at[d], send_sem=send_sem.at[d],
                recv_sem=send_sem.at[d], device_id=next_id, device_id_type=MESH,
            ).wait_send()


def write_out(adjoint, gradient, adjoint_hbm, gradient_hbm, sem):
    copies = [
        pltpu.make_async_copy(adjoint, adjoint_hbm, sem.at[0]),
        pltpu.make_async_copy(gradient, gradient_hbm, sem.at[1]),
    ]
    for copy in copies:
        copy.start()
    for copy in copies:
        copy.wait()


def solution(mesh):
    ranks, groups = mesh.shape["cells"], mesh.shape["ens"]
    assert (ranks * groups) & (ranks * groups - 1) == 0

    def body(later_adjoint, coupling, diag_inverse, sensitivity, well_cells, well_misfit, block_map):
        members, unknowns, planes, columns, layers = later_adjoint.shape
        params = sensitivity.shape[-1]
        rows = planes * columns
        blk_dev = 4
        blocks = ranks * blk_dev
        fields = members * unknowns
        sens = sensitivity.reshape(fields, rows, layers, params)
        wells = well_cells.reshape(1, -1)
        edge = (members, unknowns, columns, layers)
        any_spec = pl.BlockSpec(memory_space=pl.ANY)
        vmem_spec = pl.BlockSpec(memory_space=pltpu.VMEM)
        dma = pltpu.SemaphoreType.DMA
        adjoint, gradient = pl.pallas_call(
            functools.partial(kernel, ranks, groups, blocks),
            out_shape=(
                pltpu.VMEM(later_adjoint.shape, F32),
                pltpu.VMEM((blk_dev, params), F32),
            ),
            in_specs=[any_spec] * 7,
            out_specs=(vmem_spec, vmem_spec),
            scratch_shapes=[
                pltpu.VMEM(later_adjoint.shape, F32),
                pltpu.VMEM(coupling.shape, BF16),
                pltpu.VMEM(diag_inverse.shape, BF16),
                pltpu.VMEM(sens.shape, BF16),
                pltpu.VMEM(wells.shape, jnp.int32),
                pltpu.VMEM(well_misfit.shape, F32),
                pltpu.VMEM(block_map.shape, jnp.int32),
                pltpu.VMEM(later_adjoint.shape, F32),
                pltpu.VMEM((2, 4 + unknowns) + edge, F32),
                pltpu.VMEM((2, 4 + unknowns) + edge, F32),
                pltpu.VMEM((2,) + edge, F32),
                pltpu.VMEM((2,) + edge, F32),
                pltpu.VMEM(later_adjoint.shape, F32),
                pltpu.VMEM((planes, columns, blocks, layers), BF16),
                pltpu.VMEM((ranks, blk_dev, params), F32),
                pltpu.VMEM((ranks * groups, blk_dev, params), F32),
                dma((8,)),
                dma((2, 5, members)),
                dma((2,)),
                dma,
                dma,
                pltpu.SemaphoreType.REGULAR,
            ],
            compiler_params=pltpu.CompilerParams(collective_id=0, has_side_effects=True),
        )(later_adjoint, coupling, diag_inverse, sens, wells, well_misfit, block_map)
        return pl.pallas_call(
            write_out,
            out_shape=(
                jax.ShapeDtypeStruct(adjoint.shape, F32),
                jax.ShapeDtypeStruct(gradient.shape, F32),
            ),
            in_specs=[vmem_spec] * 2,
            out_specs=(any_spec, any_spec),
            scratch_shapes=[dma((2,))],
        )(*[pltpu.with_memory_space_constraint(a, pltpu.VMEM) for a in (adjoint, gradient)])

    placed = (
        P("ens", None, "cells", None, None),
        P("ens", None, None, None, "cells", None, None),
        P("ens", None, None, "cells", None, None),
        P("ens", None, "cells", None, None, None),
        P(),
        P("ens", None, None),
        P("cells", None, None),
    )
    return jax.shard_map(
        body,
        mesh=mesh,
        in_specs=placed,
        out_specs=(P("ens", None, "cells", None, None), P("cells", None)),
        check_vma=False,
    )
```

```python
import functools

import jax
import jax.numpy as jnp
from jax import lax
from jax.experimental import pallas as pl
from jax.experimental.pallas import tpu as pltpu
from jax.sharding import PartitionSpec as P

ITERS = 4
ORDER = (0, 1, 4, 3, 2, 5, 6)
MESH = pl.DeviceIdType.MESH
F32 = jnp.float32
BF16 = jnp.bfloat16


def for_each(count, step):
    if count <= 64:
        for i in range(count):
            step(i)
    else:
        def body(i, carry):
            step(i)
            return carry

        lax.fori_loop(0, count, body, 0)


def split(value):
    high = value.astype(BF16).astype(F32)
    return high, value - high


def kernel(
    ranks, groups, blocks,
    later_hbm, coup_hbm, diag_hbm, sens_hbm, wells_hbm, misfit_hbm, map_hbm,
    adj, got_out,
    later, coup, diag, sens, wells, misfit, bmap, source,
    out_buf, in_buf, mid_edge, last_edge, left, mask, part, got,
    load_sem, recv_sem, send_sem, part_ssem, part_rsem, here_sem, free_sem,
):
    members, unknowns, planes, columns, layers = later.shape
    rows = planes * columns
    count = rows * layers
    devices = ranks * groups
    blk_dev = blocks // ranks
    fields = members * unknowns
    me_c = lax.axis_index("cells")
    me_e = lax.axis_index("ens")
    me = me_c * groups + me_e
    assert planes >= 2

    loads = [
        pltpu.make_async_copy(src, dst, load_sem.at[i])
        for i, (src, dst) in enumerate(
            [
                (wells_hbm, wells), (misfit_hbm, misfit), (later_hbm, later), (diag_hbm, diag),
                (coup_hbm.at[:, 0:2], coup.at[:, 0:2]), (coup_hbm.at[:, 2:6], coup.at[:, 2:6]),
                (map_hbm, bmap), (sens_hbm, sens),
            ]
        )
    ]
    for i in ORDER:
        loads[i].start()

    barrier = pltpu.get_barrier_semaphore()
    has = (me_c > 0, me_c < ranks - 1)
    next_id = (jnp.minimum(me_c + 1, ranks - 1), me_e)
    prev_id = (jnp.maximum(me_c - 1, 0), me_e)
    target = (prev_id, next_id)
    is_root = me == 0

    def greet(who):
        pl.semaphore_signal(barrier, inc=1, device_id=who, device_id_type=MESH)

    for d in range(2):
        @pl.when(has[d])
        def _(d=d):
            greet(target[d])

    @pl.when(is_root)
    def _():
        for_each(devices - 1, lambda i: greet(((i + 1) // groups, (i + 1) % groups)))

    def greeted():
        known = [jnp.where(flag, 1, 0) for flag in (has[0], has[1], jnp.logical_not(is_root))]
        pl.semaphore_wait(barrier, known[0] + known[1] + known[2])

    def report():
        @pl.when(jnp.logical_not(is_root))
        def _():
            pl.semaphore_signal(here_sem, inc=1, device_id=(0, 0), device_id_type=MESH)

    def release():
        @pl.when(is_root)
        def _():
            pl.semaphore_wait(here_sem, devices - 1)
            for_each(devices - 1, lambda i: pl.semaphore_signal(
                free_sem, inc=1, device_id=((i + 1) // groups, (i + 1) % groups), device_id_type=MESH,
            ))

    def released():
        @pl.when(jnp.logical_not(is_root))
        def _():
            pl.semaphore_wait(free_sem, 1)

    edge_at = (0, planes - 1)
    turn = lax.rem(me_c, 4)
    patient = (turn == 0, turn == 3)
    GAIN = 4

    def remote(d, src, dst, sem):
        return pltpu.make_async_remote_copy(
            src_ref=src, dst_ref=dst, send_sem=send_sem.at[d], recv_sem=sem,
            device_id=target[d], device_id_type=MESH,
        )

    def value_copy(d, slot, m):
        return remote(d, out_buf.at[d, slot, m], in_buf.at[1 - d, slot, m], recv_sem.at[1 - d, slot, m])

    def gain_copy(d, m):
        both = pl.ds(GAIN, unknowns)
        return remote(d, out_buf.at[d, both, m], in_buf.at[1 - d, both, m], recv_sem.at[1 - d, GAIN, m])

    def value_wait(d, slot, m):
        pltpu.make_async_remote_copy(
            src_ref=out_buf.at[d, slot, m], dst_ref=in_buf.at[d, slot, m], send_sem=send_sem.at[d],
            recv_sem=recv_sem.at[d, slot, m], device_id=next_id, device_id_type=MESH,
        ).wait_recv()

    def gain_wait(d, m):
        both = pl.ds(GAIN, unknowns)
        pltpu.make_async_remote_copy(
            src_ref=out_buf.at[d, both, m], dst_ref=in_buf.at[d, both, m], send_sem=send_sem.at[d],
            recv_sem=recv_sem.at[d, GAIN, m], device_id=next_id, device_id_type=MESH,
        ).wait_recv()

    for d in range(2):
        @pl.when(jnp.logical_not(has[d]))
        def _(d=d):
            in_buf[d] = jnp.zeros(in_buf.shape[1:], F32)

    loads[0].wait()
    loads[1].wait()
    total_wells = wells.shape[1]
    rel = wells[...] - me_c * count
    row_lo = lax.broadcasted_iota(jnp.int32, (rows, total_wells), 0) * layers
    in_row = (rel >= row_lo) & (rel < row_lo + layers)
    lane = wells[...] & (layers - 1)
    at_lane = lax.broadcasted_iota(jnp.int32, (layers, total_wells), 0) == lane
    at_lane = jnp.where(at_lane, 1.0, 0.0).astype(BF16)
    parts = [[], [], []]
    for m in range(members):
        for u in range(unknowns):
            rest = jnp.broadcast_to(misfit[m, u : u + 1, :], (rows, total_wells))
            rest = jnp.where(in_row, rest, 0.0)
            for i in range(3):
                high, rest = split(rest)
                parts[i].append(high.astype(BF16))
    injected = jnp.zeros((fields * rows, layers), F32)
    for piece in parts:
        injected = injected + lax.dot_general(
            jnp.concatenate(piece, axis=0), at_lane, (((1,), (1,)), ((), ())),
            preferred_element_type=F32,
        )
    loads[2].wait()
    source[...] = later[...] + injected.reshape(later.shape)

    def weighed(weights, values):
        out = None
        for w in range(unknowns):
            term = weights(w) * values[w][None]
            out = term if out is None else out + term
        return out

    def inverse(m, rhs):
        return weighed(lambda w: diag[m, w].astype(F32), rhs)

    loads[3].wait()
    loads[4].wait()

    def own_gain(d, m, values):
        return weighed(lambda w: out_buf[d, GAIN + w, m], values)

    def far_gain(d, m, values):
        return weighed(lambda w: in_buf[d, GAIN + w, m], values)

    for m in range(members):
        for d in range(2):
            at = edge_at[d]
            for w in range(unknowns):
                out_buf[d, GAIN + w, m] = weighed(
                    lambda u: coup[m, 1 - d, u, :, at].astype(F32), diag[m, w, :, at].astype(F32)
                )
    edge = [[None, None] for _ in range(members)]
    for m in range(members):
        for d in range(2):
            edge[m][d] = own_gain(d, m, source[m, :, edge_at[d]])
            out_buf[d, 0, m] = edge[m][d]
    greeted()

    def send(d, copy, when):
        @pl.when(has[d] & when if when is not None else has[d])
        def _():
            copy.start()

    hasty = tuple(jnp.logical_not(p) for p in patient)
    for m in range(members):
        for d in range(2):
            send(d, value_copy(d, 0, m), None)
    report()

    now = [inverse(m, source[m]) for m in range(members)]

    lane_at = lax.broadcasted_iota(jnp.int32, (unknowns, planes, columns, layers), 3)
    col_at = lax.broadcasted_iota(jnp.int32, (unknowns, planes, columns, layers), 2)

    def product(m, k, value, lo, hi):
        return weighed(lambda u: coup[m, k, u, :, lo:hi].astype(F32), value[:, lo:hi])

    def inside(m, value):
        moved = pltpu.roll(product(m, 2, value, 0, planes), 1, 2)
        total = jnp.where(col_at == 0, 0.0, moved)
        moved = pltpu.roll(product(m, 3, value, 0, planes), columns - 1, 2)
        total = total + jnp.where(col_at == columns - 1, 0.0, moved)
        moved = pltpu.roll(product(m, 4, value, 0, planes), 1, 3)
        total = total + jnp.where(lane_at == 0, 0.0, moved)
        moved = pltpu.roll(product(m, 5, value, 0, planes), layers - 1, 3)
        total = total + jnp.where(lane_at == layers - 1, 0.0, moved)
        up = product(m, 0, value, 0, planes - 1)
        down = product(m, 1, value, 1, planes)
        nothing = jnp.zeros((unknowns, 1, columns, layers), F32)
        total = total + jnp.concatenate([nothing, up], axis=1)
        total = total + jnp.concatenate([down, nothing], axis=1)
        return source[m] - total

    def ahead(d, slot, m, rest):
        out_buf[d, slot, m] = own_gain(d, m, rest[:, edge_at[d]])

    def subtract(rest, below, above):
        first_plane = rest[:, 0] - below
        last_plane = rest[:, planes - 1] - above
        return jnp.concatenate(
            [first_plane[:, None], rest[:, 1 : planes - 1], last_plane[:, None]], axis=1
        ) if planes > 2 else jnp.stack([first_plane, last_plane], axis=1)

    loads[5].wait()
    loads[7].start()
    rest = [inside(m, now[m]) for m in range(members)]
    for m in range(members):
        for d in range(2):
            @pl.when(hasty[d])
            def _(d=d, m=m):
                ahead(d, 1, m, rest[m])

            send(d, value_copy(d, 1, m), hasty[d])

    loads[6].wait()
    ids = lax.broadcasted_iota(jnp.int32, (blocks, layers), 0)
    for x in range(planes):
        for y in range(columns):
            hit = jnp.where(bmap[x, y : y + 1, :] == ids, 1.0, 0.0)
            mask[x, y] = hit.astype(BF16)

    for m in range(members):
        for d in range(2):
            send(d, gain_copy(d, m), hasty[d])

    first_edge = edge
    second_edge = [[None, None] for _ in range(members)]
    for m in range(members):
        for d in range(2):
            @pl.when(has[d])
            def _(d=d, m=m):
                value_wait(d, 0, m)
        given = subtract(rest[m], in_buf[0, 0, m], in_buf[1, 0, m])
        for d in range(2):
            second_edge[m][d] = own_gain(d, m, given[:, edge_at[d]])

            @pl.when(patient[d])
            def _(d=d, m=m):
                out_buf[d, 1, m] = second_edge[m][d]

            send(d, value_copy(d, 1, m), patient[d])
        now[m] = inverse(m, given)
        rest[m] = inside(m, now[m])
        for d in range(2):
            ahead(d, 2, m, rest[m])
            send(d, value_copy(d, 2, m), None)
    for m in range(members):
        for d in range(2):
            send(d, gain_copy(d, m), patient[d])

    for m in range(members):
        for d in range(2):
            @pl.when(has[d])
            def _(d=d, m=m):
                value_wait(d, 1, m)

            @pl.when(has[d] & hasty[d])
            def _(d=d, m=m):
                gain_wait(d, m)

            @pl.when(hasty[d])
            def _(d=d, m=m):
                mid_edge[d, m] = in_buf[d, 1, m] - far_gain(d, m, first_edge[m][d])

            @pl.when(patient[d])
            def _(d=d, m=m):
                mid_edge[d, m] = in_buf[d, 1, m]

        given = subtract(rest[m], mid_edge[0, m], mid_edge[1, m])
        for d in range(2):
            last_edge[d, m] = own_gain(d, m, given[:, edge_at[d]])
        now[m] = inverse(m, given)
        rest[m] = inside(m, now[m])
        for d in range(2):
            ahead(d, 3, m, rest[m])
            send(d, value_copy(d, 3, m), None)

    release()

    for m in range(members):
        for d in range(2):
            @pl.when(has[d])
            def _(d=d, m=m):
                value_wait(d, 2, m)

            @pl.when(has[d] & patient[d])
            def _(d=d, m=m):
                gain_wait(d, m)

        came_in = [in_buf[d, 2, m] - far_gain(d, m, second_edge[m][d]) for d in range(2)]
        now[m] = inverse(m, subtract(rest[m], *came_in))
        left[m] = inside(m, now[m])

    loads[7].wait()

    def finish(d, total, batch):
        at = d * (planes - 1)
        for start in range(0, members, batch):
            these = range(start, min(start + batch, members))
            for m in these:
                @pl.when(jnp.where(d == 0, me_c > 0, me_c < ranks - 1))
                def _(m=m):
                    value_wait(d, 3, m)

            for m in these:
                came_in = in_buf[d, 3, m] - far_gain(d, m, last_edge[d, m])
                value = weighed(lambda w: diag[m, w, :, at].astype(F32), left[m, :, at] - came_in)
                adj[m, :, at] = value
            total = gather(at, total, these)
        return total

    def gather(at, total, these):
        def field(i, total):
            m, u = i // unknowns, i % unknowns
            pieces = split(adj[m, u, at])
            lhs = []
            for value in pieces:
                part_lhs = []
                for y in range(columns):
                    wide = jnp.broadcast_to(value[y : y + 1], (16, layers)).astype(BF16)
                    wide = jnp.concatenate([wide] * (blocks // 16), axis=0)
                    part_lhs.append(mask[at, y] * wide)
                lhs.append(jnp.concatenate(part_lhs, axis=1))
            lhs = jnp.concatenate(lhs, axis=0)
            rhs = sens[i, pl.ds(at * columns, columns)].reshape(columns * layers, sens.shape[-1])
            return total + jnp.dot(lhs, rhs, preferred_element_type=F32)

        if blocks <= 64:
            for i in range(these[0] * unknowns, (these[-1] + 1) * unknowns):
                total = field(i, total)
            return total
        return lax.fori_loop(these[0] * unknowns, (these[-1] + 1) * unknowns, field, total)

    close = lax.rem(me_c + 1, 2)
    total = jnp.zeros((2 * blocks, sens.shape[-1]), F32)
    total = finish(close, total, members)
    for x in range(1, planes - 1):
        for m in range(members):
            adj[m, :, x] = weighed(lambda w: diag[m, w, :, x].astype(F32), left[m, :, x])
        total = gather(x, total, range(members))
    total = finish(1 - close, total, 1)
    total = total[:blocks] + total[blocks:]
    for c in range(ranks):
        part[c] = total[c * blk_dev : (c + 1) * blk_dev]
    got[me] = part[me_c]

    def part_copy(c, e):
        return pltpu.make_async_remote_copy(
            src_ref=part.at[c], dst_ref=got.at[me], send_sem=part_ssem, recv_sem=part_rsem,
            device_id=(c, e), device_id_type=MESH,
        )

    released()

    def give(to):
        @pl.when(me != to)
        def _():
            part_copy(to // groups, to % groups).start()

    for_each(devices, give)
    others = got.at[pl.ds(0, devices - 1)]
    everything = pltpu.make_async_remote_copy(
        src_ref=others, dst_ref=others, send_sem=part_ssem, recv_sem=part_rsem,
        device_id=next_id, device_id_type=MESH,
    )
    everything.wait_recv()
    got_out[...] = jnp.sum(got[...], axis=0)

    everything.wait_send()
    for d in range(2):
        @pl.when(has[d])
        def _(d=d):
            pltpu.make_async_remote_copy(
                src_ref=out_buf.at[d], dst_ref=out_buf.at[d], send_sem=send_sem.at[d],
                recv_sem=send_sem.at[d], device_id=next_id, device_id_type=MESH,
            ).wait_send()


def write_out(adjoint, gradient, adjoint_hbm, gradient_hbm, sem):
    copies = [
        pltpu.make_async_copy(adjoint, adjoint_hbm, sem.at[0]),
        pltpu.make_async_copy(gradient, gradient_hbm, sem.at[1]),
    ]
    for copy in copies:
        copy.start()
    for copy in copies:
        copy.wait()


def solution(mesh):
    ranks, groups = mesh.shape["cells"], mesh.shape["ens"]
    assert (ranks * groups) & (ranks * groups - 1) == 0

    def body(later_adjoint, coupling, diag_inverse, sensitivity, well_cells, well_misfit, block_map):
        members, unknowns, planes, columns, layers = later_adjoint.shape
        params = sensitivity.shape[-1]
        rows = planes * columns
        blk_dev = 4
        blocks = ranks * blk_dev
        fields = members * unknowns
        sens = sensitivity.reshape(fields, rows, layers, params)
        wells = well_cells.reshape(1, -1)
        edge = (members, unknowns, columns, layers)
        any_spec = pl.BlockSpec(memory_space=pl.ANY)
        vmem_spec = pl.BlockSpec(memory_space=pltpu.VMEM)
        dma = pltpu.SemaphoreType.DMA
        adjoint, gradient = pl.pallas_call(
            functools.partial(kernel, ranks, groups, blocks),
            out_shape=(
                pltpu.VMEM(later_adjoint.shape, F32),
                pltpu.VMEM((blk_dev, params), F32),
            ),
            in_specs=[any_spec] * 7,
            out_specs=(vmem_spec, vmem_spec),
            scratch_shapes=[
                pltpu.VMEM(later_adjoint.shape, F32),
                pltpu.VMEM(coupling.shape, BF16),
                pltpu.VMEM(diag_inverse.shape, BF16),
                pltpu.VMEM(sens.shape, BF16),
                pltpu.VMEM(wells.shape, jnp.int32),
                pltpu.VMEM(well_misfit.shape, F32),
                pltpu.VMEM(block_map.shape, jnp.int32),
                pltpu.VMEM(later_adjoint.shape, F32),
                pltpu.VMEM((2, 4 + unknowns) + edge, F32),
                pltpu.VMEM((2, 4 + unknowns) + edge, F32),
                pltpu.VMEM((2,) + edge, F32),
                pltpu.VMEM((2,) + edge, F32),
                pltpu.VMEM(later_adjoint.shape, F32),
                pltpu.VMEM((planes, columns, blocks, layers), BF16),
                pltpu.VMEM((ranks, blk_dev, params), F32),
                pltpu.VMEM((ranks * groups, blk_dev, params), F32),
                dma((8,)),
                dma((2, 5, members)),
                dma((2,)),
                dma,
                dma,
                pltpu.SemaphoreType.REGULAR,
                pltpu.SemaphoreType.REGULAR,
            ],
            compiler_params=pltpu.CompilerParams(collective_id=0, has_side_effects=True),
        )(later_adjoint, coupling, diag_inverse, sens, wells, well_misfit, block_map)
        return pl.pallas_call(
            write_out,
            out_shape=(
                jax.ShapeDtypeStruct(adjoint.shape, F32),
                jax.ShapeDtypeStruct(gradient.shape, F32),
            ),
            in_specs=[vmem_spec] * 2,
            out_specs=(any_spec, any_spec),
            scratch_shapes=[dma((2,))],
        )(*[pltpu.with_memory_space_constraint(a, pltpu.VMEM) for a in (adjoint, gradient)])

    placed = (
        P("ens", None, "cells", None, None),
        P("ens", None, None, None, "cells", None, None),
        P("ens", None, None, "cells", None, None),
        P("ens", None, "cells", None, None, None),
        P(),
        P("ens", None, None),
        P("cells", None, None),
    )
    return jax.shard_map(
        body,
        mesh=mesh,
        in_specs=placed,
        out_specs=(P("ens", None, "cells", None, None), P("cells", None)),
        check_vma=False,
    )
```

```python
import functools

import jax
import jax.numpy as jnp
from jax import lax
from jax.experimental import pallas as pl
from jax.experimental.pallas import tpu as pltpu
from jax.sharding import PartitionSpec as P

ITERS = 4
MESH = pl.DeviceIdType.MESH
F32 = jnp.float32
BF16 = jnp.bfloat16


def for_each(start, stop, step):
    if stop - start <= 64:
        for i in range(start, stop):
            step(i)
    else:
        def body(i, carry):
            step(i)
            return carry

        lax.fori_loop(start, stop, body, 0)


def split(value):
    high = value.astype(BF16).astype(F32)
    return high, value - high


def kernel(
    ranks, groups, blocks,
    later_hbm, coup_hbm, diag_hbm, sens_hbm, wells_hbm, misfit_hbm, map_hbm,
    adj, got_out,
    later, coup, diag, sens, wells, misfit, bmap, source,
    out_buf, in_buf, mid_edge, last_edge, left, mask, head_mask, part, got,
    load_sem, recv_sem, send_sem, part_ssem, part_rsem, here_sem,
):
    members, unknowns, planes, columns, layers = later.shape
    rows = planes * columns
    count = rows * layers
    devices = ranks * groups
    blk_dev = blocks // ranks
    fields = members * unknowns
    head = 2 * blk_dev
    me_c = lax.axis_index("cells")
    me_e = lax.axis_index("ens")
    me = me_c * groups + me_e
    assert planes == 2

    close = lax.rem(me_c + 1, 2)
    open_ = 1 - close
    here, there = pl.ds(open_, 1), pl.ds(close, 1)

    def load(i, src, dst):
        return pltpu.make_async_copy(src, dst, load_sem.at[i])

    first_loads = [
        load(i, src, dst)
        for i, (src, dst) in enumerate(
            [
                (wells_hbm, wells), (misfit_hbm, misfit),
                (coup_hbm.at[:, there, :, :, here], coup.at[:, there, :, :, here]),
                (diag_hbm.at[:, :, :, here], diag.at[:, :, :, here]),
                (later_hbm.at[:, :, here], later.at[:, :, here]),
            ]
        )
    ]
    next_loads = [
        load(i, src, dst)
        for i, (src, dst) in enumerate(
            [
                (coup_hbm.at[:, here], coup.at[:, here]),
                (coup_hbm.at[:, there, :, :, there], coup.at[:, there, :, :, there]),
                (coup_hbm.at[:, 2:6], coup.at[:, 2:6]),
                (diag_hbm.at[:, :, :, there], diag.at[:, :, :, there]),
                (later_hbm.at[:, :, there], later.at[:, :, there]),
            ]
        )
    ]
    map_load = load(0, map_hbm, bmap)
    sens_load = load(1, sens_hbm, sens)
    for copy in first_loads:
        copy.start()

    barrier = pltpu.get_barrier_semaphore()
    has = (me_c > 0, me_c < ranks - 1)
    next_id = (jnp.minimum(me_c + 1, ranks - 1), me_e)
    prev_id = (jnp.maximum(me_c - 1, 0), me_e)
    target = (prev_id, next_id)
    is_root = me == 0

    def greet(who):
        pl.semaphore_signal(barrier, inc=1, device_id=who, device_id_type=MESH)

    for d in range(2):
        @pl.when(has[d])
        def _(d=d):
            greet(target[d])

    @pl.when(is_root)
    def _():
        for_each(1, devices, lambda i: greet((i // groups, i % groups)))

    def greeted():
        known = [jnp.where(flag, 1, 0) for flag in (has[0], has[1], jnp.logical_not(is_root))]
        pl.semaphore_wait(barrier, known[0] + known[1] + known[2])

    def report():
        @pl.when(jnp.logical_not(is_root))
        def _():
            pl.semaphore_signal(here_sem, inc=1, device_id=(0, 0), device_id_type=MESH)

    def release():
        @pl.when(is_root)
        def _():
            pl.semaphore_wait(here_sem, devices - 1)
            for_each(1, devices, lambda i: pl.semaphore_signal(
                here_sem, inc=1, device_id=(i // groups, i % groups), device_id_type=MESH,
            ))

    def released():
        @pl.when(jnp.logical_not(is_root))
        def _():
            pl.semaphore_wait(here_sem, 1)

    edge_at = (0, planes - 1)
    turn = lax.rem(me_c, 4)
    patient = (turn == 0, turn == 3)
    GAIN = 4

    def remote(d, src, dst, sem):
        return pltpu.make_async_remote_copy(
            src_ref=src, dst_ref=dst, send_sem=send_sem.at[d], recv_sem=sem,
            device_id=target[d], device_id_type=MESH,
        )

    def value_copy(d, slot, m):
        return remote(d, out_buf.at[d, slot, m], in_buf.at[1 - d, slot, m], recv_sem.at[1 - d, slot, m])

    def gain_copy(d, m):
        both = pl.ds(GAIN, unknowns)
        return remote(d, out_buf.at[d, both, m], in_buf.at[1 - d, both, m], recv_sem.at[1 - d, GAIN, m])

    def value_wait(d, slot, m):
        pltpu.make_async_remote_copy(
            src_ref=out_buf.at[d, slot, m], dst_ref=in_buf.at[d, slot, m], send_sem=send_sem.at[d],
            recv_sem=recv_sem.at[d, slot, m], device_id=next_id, device_id_type=MESH,
        ).wait_recv()

    def gain_wait(d, m):
        both = pl.ds(GAIN, unknowns)
        pltpu.make_async_remote_copy(
            src_ref=out_buf.at[d, both, m], dst_ref=in_buf.at[d, both, m], send_sem=send_sem.at[d],
            recv_sem=recv_sem.at[d, GAIN, m], device_id=next_id, device_id_type=MESH,
        ).wait_recv()

    for d in range(2):
        @pl.when(jnp.logical_not(has[d]))
        def _(d=d):
            in_buf[d] = jnp.zeros(in_buf.shape[1:], F32)

    first_loads[0].wait()
    first_loads[1].wait()
    total_wells = wells.shape[1]
    rel = wells[...] - me_c * count
    row = lax.broadcasted_iota(jnp.int32, (rows, total_wells), 0)
    row = row + open_ * columns
    row_lo = jnp.where(row >= rows, row - rows, row) * layers
    in_row = (rel >= row_lo) & (rel < row_lo + layers)
    lane = wells[...] & (layers - 1)
    at_lane = lax.broadcasted_iota(jnp.int32, (layers, total_wells), 0) == lane
    at_lane = jnp.where(at_lane, 1.0, 0.0).astype(BF16)
    parts = [[], [], []]
    for m in range(members):
        for u in range(unknowns):
            rest = jnp.broadcast_to(misfit[m, u : u + 1, :], (rows, total_wells))
            rest = jnp.where(in_row, rest, 0.0)
            for i in range(3):
                high, rest = split(rest)
                parts[i].append(high.astype(BF16))
    injected = jnp.zeros((fields * rows, layers), F32)
    for piece in parts:
        injected = injected + lax.dot_general(
            jnp.concatenate(piece, axis=0), at_lane, (((1,), (1,)), ((), ())),
            preferred_element_type=F32,
        )
    injected = injected.reshape(members, unknowns, planes, columns, layers)

    def weighed(weights, values):
        out = None
        for w in range(unknowns):
            term = weights(w) * values[w][None]
            out = term if out is None else out + term
        return out

    def inverse(m, rhs):
        return weighed(lambda w: diag[m, w].astype(F32), rhs)

    def own_gain(d, m, values):
        return weighed(lambda w: out_buf[d, GAIN + w, m], values)

    def far_gain(d, m, values):
        return weighed(lambda w: in_buf[d, GAIN + w, m], values)

    def set_edge(d, place):
        for m in range(members):
            for w in range(unknowns):
                out_buf[d, GAIN + w, m] = weighed(
                    lambda u: coup[m, 1 - d, u, :, d].astype(F32), diag[m, w, :, d].astype(F32)
                )
        for m in range(members):
            value = later[m, :, d] + injected[m, :, place]
            source[m, :, d] = value
            out_buf[d, 0, m] = own_gain(d, m, value)

    first_loads[2].wait()
    first_loads[3].wait()
    first_loads[4].wait()
    for copy in next_loads:
        copy.start()
    set_edge(open_, 0)
    greeted()

    def send(d, copy, when):
        @pl.when(has[d] & when if when is not None else has[d])
        def _():
            copy.start()

    hasty = tuple(jnp.logical_not(p) for p in patient)
    slow = (open_ == 0, open_ == 1)
    side = jnp.where(open_ == 1, me_c + 1, me_c - 1)
    side = jnp.clip(side, 0, ranks - 1)
    has_side = jnp.where(open_ == 1, me_c < ranks - 1, me_c > 0)

    @pl.when(has_side)
    def _():
        for m in range(members):
            pltpu.make_async_remote_copy(
                src_ref=out_buf.at[open_, 0, m], dst_ref=in_buf.at[close, 0, m],
                send_sem=send_sem.at[open_], recv_sem=recv_sem.at[close, 0, m],
                device_id=(side, me_e), device_id_type=MESH,
            ).start()

    for d in range(2):
        for m in range(members):
            send(d, gain_copy(d, m), hasty[d] & slow[d])

    for copy in next_loads:
        copy.wait()
    map_load.start()
    set_edge(close, 1)
    for d in range(2):
        for m in range(members):
            send(d, value_copy(d, 0, m), jnp.logical_not(slow[d]))
    report()

    now = [inverse(m, source[m]) for m in range(members)]

    lane_at = lax.broadcasted_iota(jnp.int32, (unknowns, planes, columns, layers), 3)
    col_at = lax.broadcasted_iota(jnp.int32, (unknowns, planes, columns, layers), 2)

    def product(m, k, value, lo, hi):
        return weighed(lambda u: coup[m, k, u, :, lo:hi].astype(F32), value[:, lo:hi])

    def inside(m, value):
        moved = pltpu.roll(product(m, 2, value, 0, planes), 1, 2)
        total = jnp.where(col_at == 0, 0.0, moved)
        moved = pltpu.roll(product(m, 3, value, 0, planes), columns - 1, 2)
        total = total + jnp.where(col_at == columns - 1, 0.0, moved)
        moved = pltpu.roll(product(m, 4, value, 0, planes), 1, 3)
        total = total + jnp.where(lane_at == 0, 0.0, moved)
        moved = pltpu.roll(product(m, 5, value, 0, planes), layers - 1, 3)
        total = total + jnp.where(lane_at == layers - 1, 0.0, moved)
        up = product(m, 0, value, 0, planes - 1)
        down = product(m, 1, value, 1, planes)
        nothing = jnp.zeros((unknowns, 1, columns, layers), F32)
        total = total + jnp.concatenate([nothing, up], axis=1)
        total = total + jnp.concatenate([down, nothing], axis=1)
        return source[m] - total

    def ahead(d, slot, m, rest):
        out_buf[d, slot, m] = own_gain(d, m, rest[:, edge_at[d]])

    def subtract(rest, below, above):
        first_plane = rest[:, 0] - below
        last_plane = rest[:, planes - 1] - above
        return jnp.concatenate(
            [first_plane[:, None], rest[:, 1 : planes - 1], last_plane[:, None]], axis=1
        ) if planes > 2 else jnp.stack([first_plane, last_plane], axis=1)

    sens_load.start()
    rest = [inside(m, now[m]) for m in range(members)]
    for m in range(members):
        for d in range(2):
            @pl.when(hasty[d])
            def _(d=d, m=m):
                ahead(d, 1, m, rest[m])

            send(d, value_copy(d, 1, m), hasty[d])

    map_load.wait()
    ids = lax.broadcasted_iota(jnp.int32, (blocks, layers), 0)
    head_ids = lax.broadcasted_iota(jnp.int32, (2 * head, layers), 0)
    head_ids = jnp.where(head_ids >= head, head_ids - head, head_ids)
    for x in range(planes):
        for y in range(columns):
            hit = jnp.where(bmap[x, y : y + 1, :] == ids, 1.0, 0.0)
            mask[x, y] = hit.astype(BF16)
            hit = jnp.where(bmap[x, y : y + 1, :] == head_ids, 1.0, 0.0)
            head_mask[x, y] = hit.astype(BF16)

    for m in range(members):
        for d in range(2):
            send(d, gain_copy(d, m), jnp.logical_not(slow[d]))

    second_edge = [[None, None] for _ in range(members)]
    for m in range(members):
        for d in range(2):
            @pl.when(has[d])
            def _(d=d, m=m):
                value_wait(d, 0, m)
        given = subtract(rest[m], in_buf[0, 0, m], in_buf[1, 0, m])
        for d in range(2):
            second_edge[m][d] = own_gain(d, m, given[:, edge_at[d]])

            @pl.when(patient[d])
            def _(d=d, m=m):
                out_buf[d, 1, m] = second_edge[m][d]

            send(d, value_copy(d, 1, m), patient[d])
        now[m] = inverse(m, given)
        rest[m] = inside(m, now[m])
        for d in range(2):
            ahead(d, 2, m, rest[m])
            send(d, value_copy(d, 2, m), None)
    for m in range(members):
        for d in range(2):
            send(d, gain_copy(d, m), patient[d])

    for m in range(members):
        for d in range(2):
            @pl.when(has[d])
            def _(d=d, m=m):
                value_wait(d, 1, m)

            @pl.when(has[d] & hasty[d])
            def _(d=d, m=m):
                gain_wait(d, m)

            @pl.when(hasty[d])
            def _(d=d, m=m):
                mid_edge[d, m] = in_buf[d, 1, m] - far_gain(d, m, out_buf[d, 0, m])

            @pl.when(patient[d])
            def _(d=d, m=m):
                mid_edge[d, m] = in_buf[d, 1, m]

        given = subtract(rest[m], mid_edge[0, m], mid_edge[1, m])
        for d in range(2):
            last_edge[d, m] = own_gain(d, m, given[:, edge_at[d]])
        now[m] = inverse(m, given)
        rest[m] = inside(m, now[m])
        for d in range(2):
            ahead(d, 3, m, rest[m])
            send(d, value_copy(d, 3, m), None)

    release()

    for m in range(members):
        for d in range(2):
            @pl.when(has[d])
            def _(d=d, m=m):
                value_wait(d, 2, m)

            @pl.when(has[d] & patient[d])
            def _(d=d, m=m):
                gain_wait(d, m)

        came_in = [in_buf[d, 2, m] - far_gain(d, m, second_edge[m][d]) for d in range(2)]
        now[m] = inverse(m, subtract(rest[m], *came_in))
        left[m] = inside(m, now[m])

    sens_load.wait()

    def settle(d, these):
        for m in these:
            @pl.when(jnp.where(d == 0, me_c > 0, me_c < ranks - 1))
            def _(m=m):
                value_wait(d, 3, m)

        for m in these:
            came_in = in_buf[d, 3, m] - far_gain(d, m, last_edge[d, m])
            value = weighed(lambda w: diag[m, w, :, d].astype(F32), left[m, :, d] - came_in)
            adj[m, :, d] = value

    def gather(at, total, these, spread):
        def field(i, total):
            pieces = split(adj[i // unknowns, i % unknowns, at])
            rhs = sens[i, pl.ds(at * columns, columns)].reshape(columns * layers, sens.shape[-1])
            return total + jnp.dot(spread(at, pieces), rhs, preferred_element_type=F32)

        bounds = these[0] * unknowns, (these[-1] + 1) * unknowns
        if blocks <= 64:
            for i in range(*bounds):
                total = field(i, total)
            return total
        return lax.fori_loop(*bounds, field, total)

    def spread_all(at, pieces):
        lhs = []
        for value in pieces:
            row = []
            for y in range(columns):
                wide = jnp.broadcast_to(value[y : y + 1], (16, layers)).astype(BF16)
                wide = jnp.concatenate([wide] * (blocks // 16), axis=0)
                row.append(mask[at, y] * wide)
            lhs.append(jnp.concatenate(row, axis=1))
        return jnp.concatenate(lhs, axis=0)

    def spread_head(at, pieces):
        row = []
        for y in range(columns):
            wide = [jnp.broadcast_to(value[y : y + 1], (head, layers)) for value in pieces]
            row.append(head_mask[at, y] * jnp.concatenate(wide, axis=0).astype(BF16))
        return jnp.concatenate(row, axis=1)

    everyone = range(members)
    params = sens.shape[-1]
    settle(close, everyone)
    total = gather(close, jnp.zeros((2 * blocks, params), F32), everyone, spread_all)
    top = jnp.zeros((2 * head, params), F32)
    for m in everyone:
        settle(open_, [m])
        top = gather(open_, top, [m], spread_head)
    top = top[:head] + top[head:] + total[:head] + total[blocks : blocks + head]
    for c in range(2):
        part[c] = top[c * blk_dev : (c + 1) * blk_dev]

    def part_copy(c, e):
        return pltpu.make_async_remote_copy(
            src_ref=part.at[c], dst_ref=got.at[me], send_sem=part_ssem, recv_sem=part_rsem,
            device_id=(c, e), device_id_type=MESH,
        )

    released()

    def give(to):
        @pl.when(me != to)
        def _():
            part_copy(to // groups, to % groups).start()

    for_each(0, 2 * groups, give)
    total = gather(open_, total, everyone, spread_all)
    total = total[:blocks] + total[blocks:]
    for c in range(2, ranks):
        part[c] = total[c * blk_dev : (c + 1) * blk_dev]
    got[me] = part[me_c]
    for_each(2 * groups, devices, give)
    others = got.at[pl.ds(0, devices - 1)]
    everything = pltpu.make_async_remote_copy(
        src_ref=others, dst_ref=others, send_sem=part_ssem, recv_sem=part_rsem,
        device_id=next_id, device_id_type=MESH,
    )
    everything.wait_recv()
    got_out[...] = jnp.sum(got[...], axis=0)

    everything.wait_send()
    for d in range(2):
        @pl.when(has[d])
        def _(d=d):
            pltpu.make_async_remote_copy(
                src_ref=out_buf.at[d], dst_ref=out_buf.at[d], send_sem=send_sem.at[d],
                recv_sem=send_sem.at[d], device_id=next_id, device_id_type=MESH,
            ).wait_send()


def write_out(adjoint, gradient, adjoint_hbm, gradient_hbm, sem):
    copies = [
        pltpu.make_async_copy(adjoint, adjoint_hbm, sem.at[0]),
        pltpu.make_async_copy(gradient, gradient_hbm, sem.at[1]),
    ]
    for copy in copies:
        copy.start()
    for copy in copies:
        copy.wait()


def solution(mesh):
    ranks, groups = mesh.shape["cells"], mesh.shape["ens"]
    assert (ranks * groups) & (ranks * groups - 1) == 0

    def body(later_adjoint, coupling, diag_inverse, sensitivity, well_cells, well_misfit, block_map):
        members, unknowns, planes, columns, layers = later_adjoint.shape
        params = sensitivity.shape[-1]
        rows = planes * columns
        blk_dev = 4
        blocks = ranks * blk_dev
        fields = members * unknowns
        sens = sensitivity.reshape(fields, rows, layers, params)
        wells = well_cells.reshape(1, -1)
        edge = (members, unknowns, columns, layers)
        any_spec = pl.BlockSpec(memory_space=pl.ANY)
        vmem_spec = pl.BlockSpec(memory_space=pltpu.VMEM)
        dma = pltpu.SemaphoreType.DMA
        adjoint, gradient = pl.pallas_call(
            functools.partial(kernel, ranks, groups, blocks),
            out_shape=(
                pltpu.VMEM(later_adjoint.shape, F32),
                pltpu.VMEM((blk_dev, params), F32),
            ),
            in_specs=[any_spec] * 7,
            out_specs=(vmem_spec, vmem_spec),
            scratch_shapes=[
                pltpu.VMEM(later_adjoint.shape, F32),
                pltpu.VMEM(coupling.shape, BF16),
                pltpu.VMEM(diag_inverse.shape, BF16),
                pltpu.VMEM(sens.shape, BF16),
                pltpu.VMEM(wells.shape, jnp.int32),
                pltpu.VMEM(well_misfit.shape, F32),
                pltpu.VMEM(block_map.shape, jnp.int32),
                pltpu.VMEM(later_adjoint.shape, F32),
                pltpu.VMEM((2, 4 + unknowns) + edge, F32),
                pltpu.VMEM((2, 4 + unknowns) + edge, F32),
                pltpu.VMEM((2,) + edge, F32),
                pltpu.VMEM((2,) + edge, F32),
                pltpu.VMEM(later_adjoint.shape, F32),
                pltpu.VMEM((planes, columns, blocks, layers), BF16),
                pltpu.VMEM((planes, columns, 4 * blk_dev, layers), BF16),
                pltpu.VMEM((ranks, blk_dev, params), F32),
                pltpu.VMEM((ranks * groups, blk_dev, params), F32),
                dma((5,)),
                dma((2, 5, members)),
                dma((2,)),
                dma,
                dma,
                pltpu.SemaphoreType.REGULAR,
            ],
            compiler_params=pltpu.CompilerParams(collective_id=0, has_side_effects=True),
        )(later_adjoint, coupling, diag_inverse, sens, wells, well_misfit, block_map)
        return pl.pallas_call(
            write_out,
            out_shape=(
                jax.ShapeDtypeStruct(adjoint.shape, F32),
                jax.ShapeDtypeStruct(gradient.shape, F32),
            ),
            in_specs=[vmem_spec] * 2,
            out_specs=(any_spec, any_spec),
            scratch_shapes=[dma((2,))],
        )(*[pltpu.with_memory_space_constraint(a, pltpu.VMEM) for a in (adjoint, gradient)])

    placed = (
        P("ens", None, "cells", None, None),
        P("ens", None, None, None, "cells", None, None),
        P("ens", None, None, "cells", None, None),
        P("ens", None, "cells", None, None, None),
        P(),
        P("ens", None, None),
        P("cells", None, None),
    )
    return jax.shard_map(
        body,
        mesh=mesh,
        in_specs=placed,
        out_specs=(P("ens", None, "cells", None, None), P("cells", None)),
        check_vma=False,
    )
```

```python
import functools

import jax
import jax.numpy as jnp
from jax import lax
from jax.experimental import pallas as pl
from jax.experimental.pallas import tpu as pltpu
from jax.sharding import PartitionSpec as P

ITERS = 4
MESH = pl.DeviceIdType.MESH
F32 = jnp.float32
BF16 = jnp.bfloat16


def for_each(start, stop, step):
    if stop - start <= 64:
        for i in range(start, stop):
            step(i)
    else:
        def body(i, carry):
            step(i)
            return carry

        lax.fori_loop(start, stop, body, 0)


def split(value):
    high = value.astype(BF16).astype(F32)
    return high, value - high


def kernel(
    ranks, groups, blocks,
    later_hbm, coup_hbm, diag_hbm, sens_hbm, wells_hbm, misfit_hbm, map_hbm,
    adj, got_out,
    later, coup, diag, sens, wells, misfit, bmap, source,
    out_buf, in_buf, mid_edge, last_edge, left, current, mask, head_mask, part, got,
    load_sem, recv_sem, send_sem, part_ssem, part_rsem, here_sem,
):
    members, unknowns, planes, columns, layers = later.shape
    rows = planes * columns
    count = rows * layers
    devices = ranks * groups
    blk_dev = blocks // ranks
    fields = members * unknowns
    head = 2 * blk_dev
    me_c = lax.axis_index("cells")
    me_e = lax.axis_index("ens")
    me = me_c * groups + me_e
    assert planes == 2

    close = lax.rem(me_c + 1, 2)
    open_ = 1 - close
    here, there = pl.ds(open_, 1), pl.ds(close, 1)

    def load(i, src, dst):
        return pltpu.make_async_copy(src, dst, load_sem.at[i])

    first_loads = [
        load(i, src, dst)
        for i, (src, dst) in enumerate(
            [
                (wells_hbm, wells), (misfit_hbm, misfit),
                (coup_hbm.at[:, there, :, :, here], coup.at[:, there, :, :, here]),
                (diag_hbm.at[:, :, :, here], diag.at[:, :, :, here]),
                (later_hbm.at[:, :, here], later.at[:, :, here]),
            ]
        )
    ]
    next_loads = [
        load(i, src, dst)
        for i, (src, dst) in enumerate(
            [
                (coup_hbm.at[:, here], coup.at[:, here]),
                (coup_hbm.at[:, there, :, :, there], coup.at[:, there, :, :, there]),
                (coup_hbm.at[:, 2:6], coup.at[:, 2:6]),
                (diag_hbm.at[:, :, :, there], diag.at[:, :, :, there]),
                (later_hbm.at[:, :, there], later.at[:, :, there]),
            ]
        )
    ]
    map_load = load(0, map_hbm, bmap)
    sens_load = load(1, sens_hbm, sens)
    barrier = pltpu.get_barrier_semaphore()
    has = (me_c > 0, me_c < ranks - 1)
    next_id = (jnp.minimum(me_c + 1, ranks - 1), me_e)
    prev_id = (jnp.maximum(me_c - 1, 0), me_e)
    target = (prev_id, next_id)
    is_root = me == 0

    def greet(who):
        pl.semaphore_signal(barrier, inc=1, device_id=who, device_id_type=MESH)

    for d in range(2):
        @pl.when(has[d])
        def _(d=d):
            greet(target[d])

    for copy in first_loads:
        copy.start()

    @pl.when(is_root)
    def _():
        for_each(1, devices, lambda i: greet((i // groups, i % groups)))

    def greeted():
        known = [jnp.where(flag, 1, 0) for flag in (has[0], has[1], jnp.logical_not(is_root))]
        pl.semaphore_wait(barrier, known[0] + known[1] + known[2])

    def report():
        @pl.when(jnp.logical_not(is_root))
        def _():
            pl.semaphore_signal(here_sem, inc=1, device_id=(0, 0), device_id_type=MESH)

    def release():
        @pl.when(is_root)
        def _():
            pl.semaphore_wait(here_sem, devices - 1)
            for_each(1, devices, lambda i: pl.semaphore_signal(
                here_sem, inc=1, device_id=(i // groups, i % groups), device_id_type=MESH,
            ))

    def released():
        @pl.when(jnp.logical_not(is_root))
        def _():
            pl.semaphore_wait(here_sem, 1)

    edge_at = (0, planes - 1)
    turn = lax.rem(me_c, 4)
    patient = (turn == 0, turn == 3)
    GAIN = 4

    def remote(d, src, dst, sem):
        return pltpu.make_async_remote_copy(
            src_ref=src, dst_ref=dst, send_sem=send_sem.at[d], recv_sem=sem,
            device_id=target[d], device_id_type=MESH,
        )

    def value_copy(d, slot, m):
        sem = recv_sem.at[1 - d, slot, 0 if slot == 2 else m]
        return remote(d, out_buf.at[d, slot, m], in_buf.at[1 - d, slot, m], sem)

    def gain_copy(d, m):
        both = pl.ds(GAIN, unknowns)
        return remote(d, out_buf.at[d, both, m], in_buf.at[1 - d, both, m], recv_sem.at[1 - d, GAIN, m])

    def value_wait(d, slot, m):
        pltpu.make_async_remote_copy(
            src_ref=out_buf.at[d, slot, m], dst_ref=in_buf.at[d, slot, m], send_sem=send_sem.at[d],
            recv_sem=recv_sem.at[d, slot, m], device_id=next_id, device_id_type=MESH,
        ).wait_recv()

    def both_wait(d, slot):
        pltpu.make_async_remote_copy(
            src_ref=out_buf.at[d, slot], dst_ref=in_buf.at[d, slot], send_sem=send_sem.at[d],
            recv_sem=recv_sem.at[d, slot, 0], device_id=next_id, device_id_type=MESH,
        ).wait_recv()

    def gain_wait(d, m):
        both = pl.ds(GAIN, unknowns)
        pltpu.make_async_remote_copy(
            src_ref=out_buf.at[d, both, m], dst_ref=in_buf.at[d, both, m], send_sem=send_sem.at[d],
            recv_sem=recv_sem.at[d, GAIN, m], device_id=next_id, device_id_type=MESH,
        ).wait_recv()

    for d in range(2):
        @pl.when(jnp.logical_not(has[d]))
        def _(d=d):
            in_buf[d] = jnp.zeros(in_buf.shape[1:], F32)

    first_loads[0].wait()
    first_loads[1].wait()
    total_wells = wells.shape[1]
    rel = wells[...] - me_c * count
    row = lax.broadcasted_iota(jnp.int32, (rows, total_wells), 0)
    row = row + open_ * columns
    row_lo = jnp.where(row >= rows, row - rows, row) * layers
    in_row = (rel >= row_lo) & (rel < row_lo + layers)
    lane = wells[...] & (layers - 1)
    at_lane = lax.broadcasted_iota(jnp.int32, (layers, total_wells), 0) == lane
    at_lane = jnp.where(at_lane, 1.0, 0.0).astype(BF16)
    parts = [[], []]
    for m in range(members):
        for u in range(unknowns):
            rest = jnp.broadcast_to(misfit[m, u : u + 1, :], (rows, total_wells))
            rest = jnp.where(in_row, rest, 0.0)
            for i in range(2):
                high, rest = split(rest)
                parts[i].append(high.astype(BF16))
    injected = jnp.zeros((fields * rows, layers), F32)
    for piece in parts:
        injected = injected + lax.dot_general(
            jnp.concatenate(piece, axis=0), at_lane, (((1,), (1,)), ((), ())),
            preferred_element_type=F32,
        )
    injected = injected.reshape(members, unknowns, planes, columns, layers)

    def weighed(weights, values):
        out = None
        for w in range(unknowns):
            term = weights(w) * values[w][None]
            out = term if out is None else out + term
        return out

    def inverse(m, rhs):
        return weighed(lambda w: diag[m, w].astype(F32), rhs)

    def own_gain(d, m, values):
        return weighed(lambda w: out_buf[d, GAIN + w, m], values)

    def far_gain(d, m, values):
        return weighed(lambda w: in_buf[d, GAIN + w, m], values)

    def set_edge(d, place):
        for m in range(members):
            for w in range(unknowns):
                out_buf[d, GAIN + w, m] = weighed(
                    lambda u: coup[m, 1 - d, u, :, d].astype(F32), diag[m, w, :, d].astype(F32)
                )
        for m in range(members):
            value = later[m, :, d] + injected[m, :, place]
            source[m, :, d] = value
            out_buf[d, 0, m] = own_gain(d, m, value)

    first_loads[2].wait()
    first_loads[3].wait()
    first_loads[4].wait()
    for copy in next_loads:
        copy.start()
    set_edge(open_, 0)
    greeted()
    report()

    def send(d, copy, when):
        @pl.when(has[d] & when if when is not None else has[d])
        def _():
            copy.start()

    hasty = tuple(jnp.logical_not(p) for p in patient)
    slow = (open_ == 0, open_ == 1)
    patient_here = (turn == 0) | (turn == 3)
    side = jnp.where(open_ == 1, me_c + 1, me_c - 1)
    side = jnp.clip(side, 0, ranks - 1)
    has_side = jnp.where(open_ == 1, me_c < ranks - 1, me_c > 0)

    def side_copy(slot, m):
        return pltpu.make_async_remote_copy(
            src_ref=out_buf.at[open_, slot, m], dst_ref=in_buf.at[close, slot, m],
            send_sem=send_sem.at[open_], recv_sem=recv_sem.at[close, slot, m],
            device_id=(side, me_e), device_id_type=MESH,
        )

    @pl.when(has_side)
    def _():
        for m in range(members):
            side_copy(0, m).start()

    for d in range(2):
        for m in range(members):
            send(d, gain_copy(d, m), hasty[d] & slow[d])

    for copy in next_loads:
        copy.wait()
    map_load.start()
    set_edge(close, 1)
    for d in range(2):
        for m in range(members):
            send(d, value_copy(d, 0, m), jnp.logical_not(slow[d]))

    now = [inverse(m, source[m]) for m in range(members)]

    lane_at = lax.broadcasted_iota(jnp.int32, (unknowns, planes, columns, layers), 3)
    col_at = lax.broadcasted_iota(jnp.int32, (unknowns, planes, columns, layers), 2)

    def product(m, k, value, lo, hi):
        return weighed(lambda u: coup[m, k, u, :, lo:hi].astype(F32), value[:, lo:hi])

    def inside(m, value):
        moved = pltpu.roll(product(m, 2, value, 0, planes), 1, 2)
        total = jnp.where(col_at == 0, 0.0, moved)
        moved = pltpu.roll(product(m, 3, value, 0, planes), columns - 1, 2)
        total = total + jnp.where(col_at == columns - 1, 0.0, moved)
        moved = pltpu.roll(product(m, 4, value, 0, planes), 1, 3)
        total = total + jnp.where(lane_at == 0, 0.0, moved)
        moved = pltpu.roll(product(m, 5, value, 0, planes), layers - 1, 3)
        total = total + jnp.where(lane_at == layers - 1, 0.0, moved)
        up = product(m, 0, value, 0, planes - 1)
        down = product(m, 1, value, 1, planes)
        nothing = jnp.zeros((unknowns, 1, columns, layers), F32)
        total = total + jnp.concatenate([nothing, up], axis=1)
        total = total + jnp.concatenate([down, nothing], axis=1)
        return source[m] - total

    def ahead(d, slot, m, rest):
        out_buf[d, slot, m] = own_gain(d, m, rest[:, edge_at[d]])

    def subtract(rest, below, above):
        first_plane = rest[:, 0] - below
        last_plane = rest[:, planes - 1] - above
        return jnp.concatenate(
            [first_plane[:, None], rest[:, 1 : planes - 1], last_plane[:, None]], axis=1
        ) if planes > 2 else jnp.stack([first_plane, last_plane], axis=1)

    sens_load.start()
    rest = [inside(m, now[m]) for m in range(members)]
    for m in range(members):
        left[m] = rest[m]
    for m in range(members):
        for d in range(2):
            @pl.when(hasty[d])
            def _(d=d, m=m):
                ahead(d, 1, m, rest[m])

            send(d, value_copy(d, 1, m), hasty[d])

    map_load.wait()
    ids = lax.broadcasted_iota(jnp.int32, (blocks, layers), 0)
    head_ids = lax.broadcasted_iota(jnp.int32, (2 * head, layers), 0)
    head_ids = jnp.where(head_ids >= head, head_ids - head, head_ids)
    for x in range(planes):
        for y in range(columns):
            hit = jnp.where(bmap[x, y : y + 1, :] == ids, 1.0, 0.0)
            mask[x, y] = hit.astype(BF16)
            hit = jnp.where(bmap[x, y : y + 1, :] == head_ids, 1.0, 0.0)
            head_mask[x, y] = hit.astype(BF16)

    for m in range(members):
        for d in range(2):
            send(d, gain_copy(d, m), jnp.logical_not(slow[d]))

    second_edge = [[None, None] for _ in range(members)]
    for m in range(members):
        @pl.when(has_side)
        def _(m=m):
            value_wait(open_, 0, m)

        @pl.when(has_side & patient_here)
        def _(m=m):
            out_buf[open_, 1, m] = own_gain(open_, m, left[m, :, open_] - in_buf[open_, 0, m])
            side_copy(1, m).start()

        for d in range(2):
            @pl.when(has[d] & jnp.logical_not(slow[d]))
            def _(d=d, m=m):
                value_wait(d, 0, m)

        given = subtract(rest[m], in_buf[0, 0, m], in_buf[1, 0, m])
        for d in range(2):
            second_edge[m][d] = own_gain(d, m, given[:, edge_at[d]])
        now[m] = inverse(m, given)
        rest[m] = inside(m, now[m])
        for d in range(2):
            ahead(d, 2, m, rest[m])
    for m in range(members):
        for d in range(2):
            send(d, value_copy(d, 2, m), None)
    for m in range(members):
        for d in range(2):
            send(d, gain_copy(d, m), patient[d])

    def inside_plane(m, d):
        def coupled(k, plane, value):
            return weighed(lambda u: coup[m, k, u, :, plane].astype(F32), value)

        value = current[m, :, d]
        moved = pltpu.roll(coupled(2, d, value), 1, 1)
        total = jnp.where(col_at[:, 0] == 0, 0.0, moved)
        moved = pltpu.roll(coupled(3, d, value), columns - 1, 1)
        total = total + jnp.where(col_at[:, 0] == columns - 1, 0.0, moved)
        moved = pltpu.roll(coupled(4, d, value), 1, 2)
        total = total + jnp.where(lane_at[:, 0] == 0, 0.0, moved)
        moved = pltpu.roll(coupled(5, d, value), layers - 1, 2)
        total = total + jnp.where(lane_at[:, 0] == layers - 1, 0.0, moved)
        total = total + coupled(1 - d, 1 - d, current[m, :, 1 - d])
        return source[m, :, d] - total

    for m in range(members):
        for d in range(2):
            @pl.when(has[d])
            def _(d=d, m=m):
                value_wait(d, 1, m)

            @pl.when(has[d] & hasty[d])
            def _(d=d, m=m):
                gain_wait(d, m)

            @pl.when(hasty[d])
            def _(d=d, m=m):
                mid_edge[d, m] = in_buf[d, 1, m] - far_gain(d, m, out_buf[d, 0, m])

            @pl.when(patient[d])
            def _(d=d, m=m):
                mid_edge[d, m] = in_buf[d, 1, m]

        given = subtract(rest[m], mid_edge[0, m], mid_edge[1, m])
        current[m] = inverse(m, given)
        for d in range(2):
            last_edge[d, m] = own_gain(d, m, given[:, edge_at[d]])
        value = inside_plane(m, open_)
        left[m, :, open_] = value
        out_buf[open_, 3, m] = own_gain(open_, m, value)

        @pl.when(has_side)
        def _(m=m):
            side_copy(3, m).start()

    for m in range(members):
        value = inside_plane(m, close)
        left[m, :, close] = value
        out_buf[close, 3, m] = own_gain(close, m, value)
        for d in range(2):
            send(d, value_copy(d, 3, m), jnp.logical_not(slow[d]))

    release()

    for d in range(2):
        @pl.when(has[d])
        def _(d=d):
            both_wait(d, 2)

    for m in range(members):
        for d in range(2):
            @pl.when(has[d] & patient[d])
            def _(d=d, m=m):
                gain_wait(d, m)

        came_in = [in_buf[d, 2, m] - far_gain(d, m, second_edge[m][d]) for d in range(2)]
        current[m] = inverse(m, subtract(left[m], *came_in))
        for d in range(2):
            left[m, :, d] = inside_plane(m, d) + far_gain(d, m, last_edge[d, m])

    sens_load.wait()

    def settle(d, these):
        for m in these:
            @pl.when(jnp.where(d == 0, me_c > 0, me_c < ranks - 1))
            def _(m=m):
                value_wait(d, 3, m)

        for m in these:
            given = left[m, :, d] - in_buf[d, 3, m]
            value = weighed(lambda w: diag[m, w, :, d].astype(F32), given)
            adj[m, :, d] = value

    def gather(at, total, these, spread):
        def field(i, total):
            pieces = split(adj[i // unknowns, i % unknowns, at])
            rhs = sens[i, pl.ds(at * columns, columns)].reshape(columns * layers, sens.shape[-1])
            return total + jnp.dot(spread(at, pieces), rhs, preferred_element_type=F32)

        bounds = these[0] * unknowns, (these[-1] + 1) * unknowns
        if blocks <= 64:
            for i in range(*bounds):
                total = field(i, total)
            return total
        return lax.fori_loop(*bounds, field, total)

    def spread_all(at, pieces):
        lhs = []
        for value in pieces:
            row = []
            for y in range(columns):
                wide = jnp.broadcast_to(value[y : y + 1], (16, layers)).astype(BF16)
                wide = jnp.concatenate([wide] * (blocks // 16), axis=0)
                row.append(mask[at, y] * wide)
            lhs.append(jnp.concatenate(row, axis=1))
        return jnp.concatenate(lhs, axis=0)

    def spread_head(at, pieces):
        row = []
        for y in range(columns):
            wide = [jnp.broadcast_to(value[y : y + 1], (head, layers)) for value in pieces]
            row.append(head_mask[at, y] * jnp.concatenate(wide, axis=0).astype(BF16))
        return jnp.concatenate(row, axis=1)

    everyone = range(members)
    params = sens.shape[-1]
    settle(close, everyone)
    total = gather(close, jnp.zeros((2 * blocks, params), F32), everyone, spread_all)
    top = jnp.zeros((2 * head, params), F32)
    for m in everyone:
        settle(open_, [m])
        top = gather(open_, top, [m], spread_head)
    top = top[:head] + top[head:] + total[:head] + total[blocks : blocks + head]
    for c in range(2):
        part[c] = top[c * blk_dev : (c + 1) * blk_dev]

    def part_copy(c, e):
        return pltpu.make_async_remote_copy(
            src_ref=part.at[c], dst_ref=got.at[me], send_sem=part_ssem, recv_sem=part_rsem,
            device_id=(c, e), device_id_type=MESH,
        )

    released()

    def give(to):
        @pl.when(me != to)
        def _():
            part_copy(to // groups, to % groups).start()

    for_each(0, 2 * groups, give)
    total = gather(open_, total, everyone, spread_all)
    total = total[:blocks] + total[blocks:]
    for c in range(2, ranks):
        part[c] = total[c * blk_dev : (c + 1) * blk_dev]
    got[me] = part[me_c]
    for_each(2 * groups, devices, give)
    others = got.at[pl.ds(0, devices - 1)]
    everything = pltpu.make_async_remote_copy(
        src_ref=others, dst_ref=others, send_sem=part_ssem, recv_sem=part_rsem,
        device_id=next_id, device_id_type=MESH,
    )
    everything.wait_recv()
    got_out[...] = jnp.sum(got[...], axis=0)

    everything.wait_send()
    for d in range(2):
        @pl.when(has[d])
        def _(d=d):
            pltpu.make_async_remote_copy(
                src_ref=out_buf.at[d], dst_ref=out_buf.at[d], send_sem=send_sem.at[d],
                recv_sem=send_sem.at[d], device_id=next_id, device_id_type=MESH,
            ).wait_send()


def write_out(adjoint, gradient, adjoint_hbm, gradient_hbm, sem):
    copies = [
        pltpu.make_async_copy(adjoint, adjoint_hbm, sem.at[0]),
        pltpu.make_async_copy(gradient, gradient_hbm, sem.at[1]),
    ]
    for copy in copies:
        copy.start()
    for copy in copies:
        copy.wait()


def solution(mesh):
    ranks, groups = mesh.shape["cells"], mesh.shape["ens"]
    assert (ranks * groups) & (ranks * groups - 1) == 0

    def body(later_adjoint, coupling, diag_inverse, sensitivity, well_cells, well_misfit, block_map):
        members, unknowns, planes, columns, layers = later_adjoint.shape
        params = sensitivity.shape[-1]
        rows = planes * columns
        blk_dev = 4
        blocks = ranks * blk_dev
        fields = members * unknowns
        sens = sensitivity.reshape(fields, rows, layers, params)
        wells = well_cells.reshape(1, -1)
        edge = (members, unknowns, columns, layers)
        any_spec = pl.BlockSpec(memory_space=pl.ANY)
        vmem_spec = pl.BlockSpec(memory_space=pltpu.VMEM)
        dma = pltpu.SemaphoreType.DMA
        adjoint, gradient = pl.pallas_call(
            functools.partial(kernel, ranks, groups, blocks),
            out_shape=(
                pltpu.VMEM(later_adjoint.shape, F32),
                pltpu.VMEM((blk_dev, params), F32),
            ),
            in_specs=[any_spec] * 7,
            out_specs=(vmem_spec, vmem_spec),
            scratch_shapes=[
                pltpu.VMEM(later_adjoint.shape, F32),
                pltpu.VMEM(coupling.shape, BF16),
                pltpu.VMEM(diag_inverse.shape, BF16),
                pltpu.VMEM(sens.shape, BF16),
                pltpu.VMEM(wells.shape, jnp.int32),
                pltpu.VMEM(well_misfit.shape, F32),
                pltpu.VMEM(block_map.shape, jnp.int32),
                pltpu.VMEM(later_adjoint.shape, F32),
                pltpu.VMEM((2, 4 + unknowns) + edge, F32),
                pltpu.VMEM((2, 4 + unknowns) + edge, F32),
                pltpu.VMEM((2,) + edge, F32),
                pltpu.VMEM((2,) + edge, F32),
                pltpu.VMEM(later_adjoint.shape, F32),
                pltpu.VMEM(later_adjoint.shape, F32),
                pltpu.VMEM((planes, columns, blocks, layers), BF16),
                pltpu.VMEM((planes, columns, 4 * blk_dev, layers), BF16),
                pltpu.VMEM((ranks, blk_dev, params), F32),
                pltpu.VMEM((ranks * groups, blk_dev, params), F32),
                dma((5,)),
                dma((2, 5, members)),
                dma((2,)),
                dma,
                dma,
                pltpu.SemaphoreType.REGULAR,
            ],
            compiler_params=pltpu.CompilerParams(collective_id=0, has_side_effects=True),
        )(later_adjoint, coupling, diag_inverse, sens, wells, well_misfit, block_map)
        return pl.pallas_call(
            write_out,
            out_shape=(
                jax.ShapeDtypeStruct(adjoint.shape, F32),
                jax.ShapeDtypeStruct(gradient.shape, F32),
            ),
            in_specs=[vmem_spec] * 2,
            out_specs=(any_spec, any_spec),
            scratch_shapes=[dma((2,))],
        )(*[pltpu.with_memory_space_constraint(a, pltpu.VMEM) for a in (adjoint, gradient)])

    placed = (
        P("ens", None, "cells", None, None),
        P("ens", None, None, None, "cells", None, None),
        P("ens", None, None, "cells", None, None),
        P("ens", None, "cells", None, None, None),
        P(),
        P("ens", None, None),
        P("cells", None, None),
    )
    return jax.shard_map(
        body,
        mesh=mesh,
        in_specs=placed,
        out_specs=(P("ens", None, "cells", None, None), P("cells", None)),
        check_vma=False,
    )
```

```python
import functools

import jax
import jax.numpy as jnp
from jax import lax
from jax.experimental import pallas as pl
from jax.experimental.pallas import tpu as pltpu
from jax.sharding import PartitionSpec as P

ITERS = 4
MESH = pl.DeviceIdType.MESH
F32 = jnp.float32
BF16 = jnp.bfloat16


def for_each(start, stop, step):
    if stop - start <= 64:
        for i in range(start, stop):
            step(i)
    else:
        def body(i, carry):
            step(i)
            return carry

        lax.fori_loop(start, stop, body, 0)


def split(value):
    high = value.astype(BF16).astype(F32)
    return high, value - high


def kernel(
    ranks, groups, blocks,
    later_hbm, coup_hbm, diag_hbm, sens_hbm, wells_hbm, misfit_hbm, map_hbm,
    adj, got_out,
    later, coup, diag, sens, wells, misfit, bmap, source,
    out_buf, in_buf, mid_edge, last_edge, left, current, mask, head_mask, part, got,
    load_sem, recv_sem, send_sem, part_rsem, here_sem,
):
    members, unknowns, planes, columns, layers = later.shape
    rows = planes * columns
    count = rows * layers
    devices = ranks * groups
    blk_dev = blocks // ranks
    fields = members * unknowns
    head = 2 * blk_dev
    me_c = lax.axis_index("cells")
    me_e = lax.axis_index("ens")
    me = me_c * groups + me_e
    assert planes == 2

    close = lax.rem(me_c + 1, 2)
    open_ = 1 - close
    here, there = pl.ds(open_, 1), pl.ds(close, 1)

    def load(i, src, dst):
        return pltpu.make_async_copy(src, dst, load_sem.at[i])

    first_loads = [
        load(i, src, dst)
        for i, (src, dst) in enumerate(
            [
                (wells_hbm, wells), (misfit_hbm, misfit),
                (coup_hbm.at[:, there, :, :, here], coup.at[:, there, :, :, here]),
                (diag_hbm.at[:, :, :, here], diag.at[:, :, :, here]),
                (later_hbm.at[:, :, here], later.at[:, :, here]),
            ]
        )
    ]
    next_loads = [
        load(i, src, dst)
        for i, (src, dst) in enumerate(
            [
                (coup_hbm.at[:, here], coup.at[:, here]),
                (coup_hbm.at[:, there, :, :, there], coup.at[:, there, :, :, there]),
                (coup_hbm.at[:, 2:6], coup.at[:, 2:6]),
                (diag_hbm.at[:, :, :, there], diag.at[:, :, :, there]),
                (later_hbm.at[:, :, there], later.at[:, :, there]),
            ]
        )
    ]
    map_load = load(0, map_hbm, bmap)
    sens_load = load(1, sens_hbm, sens)
    barrier = pltpu.get_barrier_semaphore()
    has = (me_c > 0, me_c < ranks - 1)
    next_id = (jnp.minimum(me_c + 1, ranks - 1), me_e)
    prev_id = (jnp.maximum(me_c - 1, 0), me_e)
    target = (prev_id, next_id)
    is_root = me == 0

    def greet(who):
        pl.semaphore_signal(barrier, inc=1, device_id=who, device_id_type=MESH)

    for d in range(2):
        @pl.when(has[d])
        def _(d=d):
            greet(target[d])

    for copy in first_loads:
        copy.start()

    @pl.when(is_root)
    def _():
        for_each(1, devices, lambda i: greet((i // groups, i % groups)))

    def greeted():
        known = [jnp.where(flag, 1, 0) for flag in (has[0], has[1], jnp.logical_not(is_root))]
        pl.semaphore_wait(barrier, known[0] + known[1] + known[2])

    def report():
        @pl.when(jnp.logical_not(is_root))
        def _():
            pl.semaphore_signal(here_sem, inc=1, device_id=(0, 0), device_id_type=MESH)

    def release():
        @pl.when(is_root)
        def _():
            pl.semaphore_wait(here_sem, devices - 1)
            for_each(1, devices, lambda i: pl.semaphore_signal(
                here_sem, inc=1, device_id=(i // groups, i % groups), device_id_type=MESH,
            ))

    def released():
        @pl.when(jnp.logical_not(is_root))
        def _():
            pl.semaphore_wait(here_sem, 1)

    edge_at = (0, planes - 1)
    turn = lax.rem(me_c, 4)
    patient = (turn == 0, turn == 3)
    GAIN = 4

    def remote(d, src, dst, sem):
        return pltpu.make_async_remote_copy(
            src_ref=src, dst_ref=dst, send_sem=send_sem.at[d], recv_sem=sem,
            device_id=target[d], device_id_type=MESH,
        )

    def place(slot, m):
        return 0 if slot == 2 else 1 + {0: 0, 1: 1, 3: 2, GAIN: 3}[slot] * members + m

    def value_copy(d, slot, m):
        sem = recv_sem.at[1 - d, place(slot, m)]
        return remote(d, out_buf.at[d, slot, m], in_buf.at[1 - d, slot, m], sem)

    def gain_copy(d, m):
        both = pl.ds(GAIN, unknowns)
        return remote(d, out_buf.at[d, both, m], in_buf.at[1 - d, both, m], recv_sem.at[1 - d, place(GAIN, m)])

    def value_wait(d, slot, m):
        pltpu.make_async_remote_copy(
            src_ref=out_buf.at[d, slot, m], dst_ref=in_buf.at[d, slot, m], send_sem=send_sem.at[d],
            recv_sem=recv_sem.at[d, place(slot, m)], device_id=next_id, device_id_type=MESH,
        ).wait_recv()

    def both_wait(d, slot):
        pltpu.make_async_remote_copy(
            src_ref=out_buf.at[d, slot], dst_ref=in_buf.at[d, slot], send_sem=send_sem.at[d],
            recv_sem=recv_sem.at[d, place(slot, 0)], device_id=next_id, device_id_type=MESH,
        ).wait_recv()

    def gain_wait(d, m):
        both = pl.ds(GAIN, unknowns)
        pltpu.make_async_remote_copy(
            src_ref=out_buf.at[d, both, m], dst_ref=in_buf.at[d, both, m], send_sem=send_sem.at[d],
            recv_sem=recv_sem.at[d, place(GAIN, m)], device_id=next_id, device_id_type=MESH,
        ).wait_recv()

    for d in range(2):
        @pl.when(jnp.logical_not(has[d]))
        def _(d=d):
            in_buf[d] = jnp.zeros(in_buf.shape[1:], F32)

    first_loads[0].wait()
    first_loads[1].wait()
    total_wells = wells.shape[1]
    rel = wells[...] - me_c * count
    row = lax.broadcasted_iota(jnp.int32, (rows, total_wells), 0)
    row = row + open_ * columns
    row_lo = jnp.where(row >= rows, row - rows, row) * layers
    in_row = (rel >= row_lo) & (rel < row_lo + layers)
    lane = wells[...] & (layers - 1)
    at_lane = lax.broadcasted_iota(jnp.int32, (layers, total_wells), 0) == lane
    at_lane = jnp.where(at_lane, 1.0, 0.0).astype(BF16)
    parts = [[], []]
    for m in range(members):
        for u in range(unknowns):
            rest = jnp.broadcast_to(misfit[m, u : u + 1, :], (rows, total_wells))
            rest = jnp.where(in_row, rest, 0.0)
            for i in range(2):
                high, rest = split(rest)
                parts[i].append(high.astype(BF16))
    injected = jnp.zeros((fields * rows, layers), F32)
    for piece in parts:
        injected = injected + lax.dot_general(
            jnp.concatenate(piece, axis=0), at_lane, (((1,), (1,)), ((), ())),
            preferred_element_type=F32,
        )
    injected = injected.reshape(members, unknowns, planes, columns, layers)

    def weighed(weights, values):
        out = None
        for w in range(unknowns):
            term = weights(w) * values[w][None]
            out = term if out is None else out + term
        return out

    def inverse(m, rhs):
        return weighed(lambda w: diag[m, w].astype(F32), rhs)

    def own_gain(d, m, values):
        return weighed(lambda w: out_buf[d, GAIN + w, m], values)

    def far_gain(d, m, values):
        return weighed(lambda w: in_buf[d, GAIN + w, m], values)

    def set_edge(d, place):
        for m in range(members):
            for w in range(unknowns):
                out_buf[d, GAIN + w, m] = weighed(
                    lambda u: coup[m, 1 - d, u, :, d].astype(F32), diag[m, w, :, d].astype(F32)
                )
        for m in range(members):
            value = later[m, :, d] + injected[m, :, place]
            source[m, :, d] = value
            out_buf[d, 0, m] = own_gain(d, m, value)

    first_loads[2].wait()
    first_loads[3].wait()
    first_loads[4].wait()
    for copy in next_loads:
        copy.start()
    set_edge(open_, 0)
    greeted()
    report()

    def send(d, copy, when):
        @pl.when(has[d] & when if when is not None else has[d])
        def _():
            copy.start()

    hasty = tuple(jnp.logical_not(p) for p in patient)
    slow = (open_ == 0, open_ == 1)
    patient_here = (turn == 0) | (turn == 3)
    side = jnp.where(open_ == 1, me_c + 1, me_c - 1)
    side = jnp.clip(side, 0, ranks - 1)
    has_side = jnp.where(open_ == 1, me_c < ranks - 1, me_c > 0)

    def side_copy(slot, m):
        return pltpu.make_async_remote_copy(
            src_ref=out_buf.at[open_, slot, m], dst_ref=in_buf.at[close, slot, m],
            send_sem=send_sem.at[open_], recv_sem=recv_sem.at[close, place(slot, m)],
            device_id=(side, me_e), device_id_type=MESH,
        )

    @pl.when(has_side)
    def _():
        for m in range(members):
            side_copy(0, m).start()

    for d in range(2):
        for m in range(members):
            send(d, gain_copy(d, m), hasty[d] & slow[d])

    for copy in next_loads:
        copy.wait()
    map_load.start()
    set_edge(close, 1)
    for d in range(2):
        for m in range(members):
            send(d, value_copy(d, 0, m), jnp.logical_not(slow[d]))

    now = [inverse(m, source[m]) for m in range(members)]

    lane_at = lax.broadcasted_iota(jnp.int32, (unknowns, planes, columns, layers), 3)
    col_at = lax.broadcasted_iota(jnp.int32, (unknowns, planes, columns, layers), 2)

    def product(m, k, value, lo, hi):
        return weighed(lambda u: coup[m, k, u, :, lo:hi].astype(F32), value[:, lo:hi])

    def inside(m, value):
        moved = pltpu.roll(product(m, 2, value, 0, planes), 1, 2)
        total = jnp.where(col_at == 0, 0.0, moved)
        moved = pltpu.roll(product(m, 3, value, 0, planes), columns - 1, 2)
        total = total + jnp.where(col_at == columns - 1, 0.0, moved)
        moved = pltpu.roll(product(m, 4, value, 0, planes), 1, 3)
        total = total + jnp.where(lane_at == 0, 0.0, moved)
        moved = pltpu.roll(product(m, 5, value, 0, planes), layers - 1, 3)
        total = total + jnp.where(lane_at == layers - 1, 0.0, moved)
        up = product(m, 0, value, 0, planes - 1)
        down = product(m, 1, value, 1, planes)
        nothing = jnp.zeros((unknowns, 1, columns, layers), F32)
        total = total + jnp.concatenate([nothing, up], axis=1)
        total = total + jnp.concatenate([down, nothing], axis=1)
        return source[m] - total

    def ahead(d, slot, m, rest):
        out_buf[d, slot, m] = own_gain(d, m, rest[:, edge_at[d]])

    def subtract(rest, below, above):
        first_plane = rest[:, 0] - below
        last_plane = rest[:, planes - 1] - above
        return jnp.concatenate(
            [first_plane[:, None], rest[:, 1 : planes - 1], last_plane[:, None]], axis=1
        ) if planes > 2 else jnp.stack([first_plane, last_plane], axis=1)

    sens_load.start()
    rest = [inside(m, now[m]) for m in range(members)]
    for m in range(members):
        left[m] = rest[m]
    for m in range(members):
        for d in range(2):
            @pl.when(hasty[d])
            def _(d=d, m=m):
                ahead(d, 1, m, rest[m])

            send(d, value_copy(d, 1, m), hasty[d])

    map_load.wait()
    ids = lax.broadcasted_iota(jnp.int32, (blocks, layers), 0)
    head_ids = lax.broadcasted_iota(jnp.int32, (2 * head, layers), 0)
    head_ids = jnp.where(head_ids >= head, head_ids - head, head_ids)
    for x in range(planes):
        for y in range(columns):
            hit = jnp.where(bmap[x, y : y + 1, :] == ids, 1.0, 0.0)
            mask[x, y] = hit.astype(BF16)
            hit = jnp.where(bmap[x, y : y + 1, :] == head_ids, 1.0, 0.0)
            head_mask[x, y] = hit.astype(BF16)

    for m in range(members):
        for d in range(2):
            send(d, gain_copy(d, m), jnp.logical_not(slow[d]))

    second_edge = [[None, None] for _ in range(members)]
    for m in range(members):
        @pl.when(has_side)
        def _(m=m):
            value_wait(open_, 0, m)

        @pl.when(has_side & patient_here)
        def _(m=m):
            out_buf[open_, 1, m] = own_gain(open_, m, left[m, :, open_] - in_buf[open_, 0, m])
            side_copy(1, m).start()

        for d in range(2):
            @pl.when(has[d] & jnp.logical_not(slow[d]))
            def _(d=d, m=m):
                value_wait(d, 0, m)

        given = subtract(rest[m], in_buf[0, 0, m], in_buf[1, 0, m])
        for d in range(2):
            second_edge[m][d] = own_gain(d, m, given[:, edge_at[d]])
        now[m] = inverse(m, given)
        rest[m] = inside(m, now[m])
        for d in range(2):
            ahead(d, 2, m, rest[m])
    for m in range(members):
        for d in range(2):
            send(d, value_copy(d, 2, m), None)
    for m in range(members):
        for d in range(2):
            send(d, gain_copy(d, m), patient[d])

    def inside_plane(m, d):
        def coupled(k, plane, value):
            return weighed(lambda u: coup[m, k, u, :, plane].astype(F32), value)

        value = current[m, :, d]
        moved = pltpu.roll(coupled(2, d, value), 1, 1)
        total = jnp.where(col_at[:, 0] == 0, 0.0, moved)
        moved = pltpu.roll(coupled(3, d, value), columns - 1, 1)
        total = total + jnp.where(col_at[:, 0] == columns - 1, 0.0, moved)
        moved = pltpu.roll(coupled(4, d, value), 1, 2)
        total = total + jnp.where(lane_at[:, 0] == 0, 0.0, moved)
        moved = pltpu.roll(coupled(5, d, value), layers - 1, 2)
        total = total + jnp.where(lane_at[:, 0] == layers - 1, 0.0, moved)
        total = total + coupled(1 - d, 1 - d, current[m, :, 1 - d])
        return source[m, :, d] - total

    for m in range(members):
        for d in range(2):
            @pl.when(has[d])
            def _(d=d, m=m):
                value_wait(d, 1, m)

            @pl.when(has[d] & hasty[d])
            def _(d=d, m=m):
                gain_wait(d, m)

            @pl.when(hasty[d])
            def _(d=d, m=m):
                mid_edge[d, m] = in_buf[d, 1, m] - far_gain(d, m, out_buf[d, 0, m])

            @pl.when(patient[d])
            def _(d=d, m=m):
                mid_edge[d, m] = in_buf[d, 1, m]

        given = subtract(rest[m], mid_edge[0, m], mid_edge[1, m])
        current[m] = inverse(m, given)
        for d in range(2):
            last_edge[d, m] = own_gain(d, m, given[:, edge_at[d]])
        value = inside_plane(m, open_)
        left[m, :, open_] = value
        out_buf[open_, 3, m] = own_gain(open_, m, value)

        @pl.when(has_side)
        def _(m=m):
            side_copy(3, m).start()

    for m in range(members):
        value = inside_plane(m, close)
        left[m, :, close] = value
        out_buf[close, 3, m] = own_gain(close, m, value)
        for d in range(2):
            send(d, value_copy(d, 3, m), jnp.logical_not(slow[d]))

    release()

    for d in range(2):
        @pl.when(has[d])
        def _(d=d):
            both_wait(d, 2)

    for m in range(members):
        for d in range(2):
            @pl.when(has[d] & patient[d])
            def _(d=d, m=m):
                gain_wait(d, m)

        came_in = [in_buf[d, 2, m] - far_gain(d, m, second_edge[m][d]) for d in range(2)]
        current[m] = inverse(m, subtract(left[m], *came_in))
        for d in range(2):
            left[m, :, d] = inside_plane(m, d) + far_gain(d, m, last_edge[d, m])

    sens_load.wait()

    def settle(d, these):
        for m in these:
            @pl.when(jnp.where(d == 0, me_c > 0, me_c < ranks - 1))
            def _(m=m):
                value_wait(d, 3, m)

        for m in these:
            given = left[m, :, d] - in_buf[d, 3, m]
            value = weighed(lambda w: diag[m, w, :, d].astype(F32), given)
            adj[m, :, d] = value

    def gather(at, total, these, spread):
        def field(i, total):
            pieces = split(adj[i // unknowns, i % unknowns, at])
            rhs = sens[i, pl.ds(at * columns, columns)].reshape(columns * layers, sens.shape[-1])
            return total + jnp.dot(spread(at, pieces), rhs, preferred_element_type=F32)

        bounds = these[0] * unknowns, (these[-1] + 1) * unknowns
        if blocks <= 64:
            for i in range(*bounds):
                total = field(i, total)
            return total
        return lax.fori_loop(*bounds, field, total)

    def spread_all(at, pieces):
        lhs = []
        for value in pieces:
            row = []
            for y in range(columns):
                wide = jnp.broadcast_to(value[y : y + 1], (16, layers)).astype(BF16)
                wide = jnp.concatenate([wide] * (blocks // 16), axis=0)
                row.append(mask[at, y] * wide)
            lhs.append(jnp.concatenate(row, axis=1))
        return jnp.concatenate(lhs, axis=0)

    def spread_head(at, pieces):
        row = []
        for y in range(columns):
            wide = [jnp.broadcast_to(value[y : y + 1], (head, layers)) for value in pieces]
            row.append(head_mask[at, y] * jnp.concatenate(wide, axis=0).astype(BF16))
        return jnp.concatenate(row, axis=1)

    everyone = range(members)
    params = sens.shape[-1]
    settle(close, everyone)
    total = gather(close, jnp.zeros((2 * blocks, params), F32), everyone, spread_all)
    top = jnp.zeros((2 * head, params), F32)
    for m in everyone:
        settle(open_, [m])
        top = gather(open_, top, [m], spread_head)
    top = top[:head] + top[head:] + total[:head] + total[blocks : blocks + head]
    for c in range(2):
        part[c] = top[c * blk_dev : (c + 1) * blk_dev]

    def part_copy(c, e):
        return pltpu.make_async_remote_copy(
            src_ref=part.at[c], dst_ref=got.at[me], send_sem=load_sem.at[0], recv_sem=part_rsem,
            device_id=(c, e), device_id_type=MESH,
        )

    released()

    def give(to):
        @pl.when(me != to)
        def _():
            part_copy(to // groups, to % groups).start()

    for_each(0, 2 * groups, give)
    total = gather(open_, total, everyone, spread_all)
    total = total[:blocks] + total[blocks:]
    for c in range(2, ranks):
        part[c] = total[c * blk_dev : (c + 1) * blk_dev]
    got[me] = part[me_c]
    for_each(2 * groups, devices, give)
    others = got.at[pl.ds(0, devices - 1)]
    everything = pltpu.make_async_remote_copy(
        src_ref=others, dst_ref=others, send_sem=load_sem.at[0], recv_sem=part_rsem,
        device_id=next_id, device_id_type=MESH,
    )
    everything.wait_recv()
    got_out[...] = jnp.sum(got[...], axis=0)

    everything.wait_send()
    for d in range(2):
        @pl.when(has[d])
        def _(d=d):
            pltpu.make_async_remote_copy(
                src_ref=out_buf.at[d], dst_ref=out_buf.at[d], send_sem=send_sem.at[d],
                recv_sem=send_sem.at[d], device_id=next_id, device_id_type=MESH,
            ).wait_send()


def write_out(adjoint, gradient, adjoint_hbm, gradient_hbm, sem):
    copies = [
        pltpu.make_async_copy(adjoint, adjoint_hbm, sem.at[0]),
        pltpu.make_async_copy(gradient, gradient_hbm, sem.at[1]),
    ]
    for copy in copies:
        copy.start()
    for copy in copies:
        copy.wait()


def solution(mesh):
    ranks, groups = mesh.shape["cells"], mesh.shape["ens"]
    assert (ranks * groups) & (ranks * groups - 1) == 0

    def body(later_adjoint, coupling, diag_inverse, sensitivity, well_cells, well_misfit, block_map):
        members, unknowns, planes, columns, layers = later_adjoint.shape
        params = sensitivity.shape[-1]
        rows = planes * columns
        blk_dev = 4
        blocks = ranks * blk_dev
        fields = members * unknowns
        sens = sensitivity.reshape(fields, rows, layers, params)
        wells = well_cells.reshape(1, -1)
        edge = (members, unknowns, columns, layers)
        any_spec = pl.BlockSpec(memory_space=pl.ANY)
        vmem_spec = pl.BlockSpec(memory_space=pltpu.VMEM)
        dma = pltpu.SemaphoreType.DMA
        adjoint, gradient = pl.pallas_call(
            functools.partial(kernel, ranks, groups, blocks),
            out_shape=(
                pltpu.VMEM(later_adjoint.shape, F32),
                pltpu.VMEM((blk_dev, params), F32),
            ),
            in_specs=[any_spec] * 7,
            out_specs=(vmem_spec, vmem_spec),
            scratch_shapes=[
                pltpu.VMEM(later_adjoint.shape, F32),
                pltpu.VMEM(coupling.shape, BF16),
                pltpu.VMEM(diag_inverse.shape, BF16),
                pltpu.VMEM(sens.shape, BF16),
                pltpu.VMEM(wells.shape, jnp.int32),
                pltpu.VMEM(well_misfit.shape, F32),
                pltpu.VMEM(block_map.shape, jnp.int32),
                pltpu.VMEM(later_adjoint.shape, F32),
                pltpu.VMEM((2, 4 + unknowns) + edge, F32),
                pltpu.VMEM((2, 4 + unknowns) + edge, F32),
                pltpu.VMEM((2,) + edge, F32),
                pltpu.VMEM((2,) + edge, F32),
                pltpu.VMEM(later_adjoint.shape, F32),
                pltpu.VMEM(later_adjoint.shape, F32),
                pltpu.VMEM((planes, columns, blocks, layers), BF16),
                pltpu.VMEM((planes, columns, 4 * blk_dev, layers), BF16),
                pltpu.VMEM((ranks, blk_dev, params), F32),
                pltpu.VMEM((ranks * groups, blk_dev, params), F32),
                dma((5,)),
                dma((2, 1 + 4 * members)),
                dma((2,)),
                dma,
                pltpu.SemaphoreType.REGULAR,
            ],
            compiler_params=pltpu.CompilerParams(collective_id=0, has_side_effects=True),
        )(later_adjoint, coupling, diag_inverse, sens, wells, well_misfit, block_map)
        return pl.pallas_call(
            write_out,
            out_shape=(
                jax.ShapeDtypeStruct(adjoint.shape, F32),
                jax.ShapeDtypeStruct(gradient.shape, F32),
            ),
            in_specs=[vmem_spec] * 2,
            out_specs=(any_spec, any_spec),
            scratch_shapes=[dma((2,))],
        )(*[pltpu.with_memory_space_constraint(a, pltpu.VMEM) for a in (adjoint, gradient)])

    placed = (
        P("ens", None, "cells", None, None),
        P("ens", None, None, None, "cells", None, None),
        P("ens", None, None, "cells", None, None),
        P("ens", None, "cells", None, None, None),
        P(),
        P("ens", None, None),
        P("cells", None, None),
    )
    return jax.shard_map(
        body,
        mesh=mesh,
        in_specs=placed,
        out_specs=(P("ens", None, "cells", None, None), P("cells", None)),
        check_vma=False,
    )
```
